32 devices in a mesh: chain: 4 (over z), inner: 8 (over y, x, core).
Axes of the slice: x: 2, y: 2, z: 4, core: 2. Of those that a mesh axis runs over, the one named last changes fastest.
Arguments:
- queries: bfloat16 [4096, 4096], P(('chain', 'inner')), may hold values from -0.75 to 0.75
- key_rows: bfloat16 [4096, 4096], P(('chain', 'inner')), may hold values from -0.75 to 0.75
- value_rows: bfloat16 [4096, 4096], P(('chain', 'inner')), may hold values from -0.75 to 0.75
- out_grad: bfloat16 [4096, 4096], P(('chain', 'inner')), may hold values from -0.75 to 0.75
- log_decay: bfloat16 [4096, 32], P(('chain', 'inner')), may hold values from -2 to 0, as said below
Outputs:
- attended: bfloat16 [4096, 4096], P(('chain', 'inner'))
- query_grad: bfloat16 [4096, 4096], P(('chain', 'inner'))
- key_grad: bfloat16 [4096, 4096], P(('chain', 'inner'))
- value_grad: bfloat16 [4096, 4096], P(('chain', 'inner'))
The draws below stay inside these ranges and needn't reach their ends.
Inputs may be any that keep to these rules, and one draw needn't show every extreme that they name: `log_decay`: every entry is negative.
All inputs are finite; a program needn't handle non-finite values.
Results may differ from the reference program's by a relative error of at most 0.0051.
Values may be sent and summed in bfloat16 or wider, within the bound.
A program may use at most 64 MiB of HBM per device.

```python
import jax
import jax.numpy as jnp
from jax import lax

HEAD_SIZE = 128
HEAD_COUNT = 32
BLOCK = 128
TOKEN_COUNT = 4096


def draw_log_decay(key, part):
    parallel_sequences = jax.random.split(key, 5)
    quick_heads = jax.random.randint(parallel_sequences[0], (HEAD_COUNT,), 0, 2) == 1
    spread = jnp.exp(jax.random.uniform(parallel_sequences[1], (HEAD_COUNT,), minval=-0.69, maxval=0.69))
    head_decay_speeds = jnp.where(quick_heads, 3.0 / BLOCK, 0.15 / TOKEN_COUNT) * spread
    decay_jitter = jax.random.uniform(parallel_sequences[2], (TOKEN_COUNT, HEAD_COUNT), minval=0.5, maxval=2.0)
    spike_token_rows = jax.random.randint(parallel_sequences[3], (3,), 0, TOKEN_COUNT)
    spike_length = jnp.log(jax.random.uniform(parallel_sequences[4], (3, HEAD_COUNT), minval=0.55, maxval=0.8))
    spike_positions = (jnp.arange(TOKEN_COUNT)[:, None] == spike_token_rows[None, :]).astype(jnp.float32)
    value_inputs = -(head_decay_speeds[None, :] * decay_jitter) + jnp.dot(spike_positions, spike_length)
    return value_inputs.astype(jnp.bfloat16)


def levels(own_key, dims, cuts, least, high):
    level, own = 1.0, jax.random.fold_in(own_key, 6)
    for axis_at, blocks in cuts:
        draws = jnp.exp(jax.random.uniform(jax.random.fold_in(own, axis_at), (blocks,), jnp.float32, least / len(cuts), high / len(cuts)))
        level = level * jnp.repeat(draws, dims[axis_at] // blocks).reshape([-1 if axis == axis_at else 1 for axis in range(len(dims))])
    return level


def bell_draw(rng, dims, width, limit, pieces=(), held_as=jnp.bfloat16):
    drawn = jax.random.normal(rng, dims, jnp.float32) * width
    if len(pieces) > 0:
        drawn = levels(rng, dims, pieces, -0.22, 0.18) * drawn
    return jnp.clip(drawn, min=-limit, max=limit).astype(held_as)


def setup_inputs(seed: int = 0) -> dict:
    key_of = jax.random.split(jax.random.key(seed), 6)
    return {
        "queries": bell_draw(key_of[0], (TOKEN_COUNT, HEAD_COUNT * HEAD_SIZE), 0.125, 0.75, ((0, 32),)),
        "key_rows": bell_draw(key_of[1], (TOKEN_COUNT, HEAD_COUNT * HEAD_SIZE), 0.125, 0.75, ((0, 32),)),
        "value_rows": bell_draw(key_of[2], (TOKEN_COUNT, HEAD_COUNT * HEAD_SIZE), 0.125, 0.75, ((0, 32),)),
        "out_grad": bell_draw(key_of[3], (TOKEN_COUNT, HEAD_COUNT * HEAD_SIZE), 0.125, 0.75, ((0, 32),)),
        "log_decay": draw_log_decay(jax.random.fold_in(key_of[5], 71), 0),
    }


def advance(state, inputs):
    factor, term = inputs
    return jnp.exp(factor) * state + term, state


def narrowed(array):
    return lax.optimization_barrier(array.astype(jnp.bfloat16)).astype(jnp.float32)


def one_head(query_head, key_head, value_head, grad_head, decay_head):
    blocks = TOKEN_COUNT // BLOCK
    highest = lax.Precision.HIGHEST
    query_f = query_head.astype(jnp.float32).reshape(blocks, BLOCK, HEAD_SIZE)
    key_f = key_head.astype(jnp.float32).reshape(blocks, BLOCK, HEAD_SIZE)
    value_f = value_head.astype(jnp.float32).reshape(blocks, BLOCK, HEAD_SIZE)
    grad_f = grad_head.astype(jnp.float32).reshape(blocks, BLOCK, HEAD_SIZE)
    cumul = jnp.cumsum(decay_head.astype(jnp.float32).reshape(blocks, BLOCK), axis=1)
    finals = cumul[:, -1]
    forward_scale = jnp.exp(cumul)[:, :, None]
    backward_scale = jnp.exp(finals[:, None] - cumul)[:, :, None]
    scaled_keys = narrowed(key_f * backward_scale)
    scaled_queries = narrowed(query_f * forward_scale)
    kv_terms = jnp.einsum("jsd,jse->jde", scaled_keys, value_f, precision=highest)
    qd_terms = jnp.einsum("jtd,jte->jde", scaled_queries, grad_f, precision=highest)
    zero_state = jnp.zeros((HEAD_SIZE, HEAD_SIZE), jnp.float32)
    _, entering = lax.scan(advance, zero_state, (finals, kv_terms))
    _, trailing = lax.scan(advance, zero_state, (finals, qd_terms), reverse=True)
    enter_narrow = narrowed(entering)
    trail_narrow = narrowed(trailing)
    positions = jnp.arange(BLOCK)
    lower = positions[:, None] >= positions[None, :]
    weights = jnp.exp(jnp.where(lower[None], cumul[:, :, None] - cumul[:, None, :], -jnp.inf))
    scores = jnp.einsum("jtd,jsd->jts", query_f, key_f, precision=highest)
    probs = narrowed(scores * weights)
    grows = narrowed(jnp.einsum("jte,jse->jts", grad_f, value_f, precision=highest) * weights)
    attended = jnp.einsum("jts,jse->jte", probs, value_f, precision=highest) + forward_scale * jnp.einsum("jtd,jde->jte", query_f, enter_narrow, precision=highest)
    query_grad = jnp.einsum("jts,jsd->jtd", grows, key_f, precision=highest) + forward_scale * jnp.einsum("jte,jde->jtd", grad_f, enter_narrow, precision=highest)
    key_grad = jnp.einsum("jts,jtd->jsd", grows, query_f, precision=highest) + backward_scale * jnp.einsum("jse,jde->jsd", value_f, trail_narrow, precision=highest)
    value_grad = jnp.einsum("jts,jte->jse", probs, grad_f, precision=highest) + backward_scale * jnp.einsum("jsd,jde->jse", key_f, trail_narrow, precision=highest)
    return tuple(item.reshape(TOKEN_COUNT, HEAD_SIZE).astype(jnp.bfloat16) for item in (attended, query_grad, key_grad, value_grad))


def head_major(array):
    return array.reshape(TOKEN_COUNT, HEAD_COUNT, HEAD_SIZE).transpose(1, 0, 2)


def token_major(array):
    return array.transpose(1, 0, 2).reshape(TOKEN_COUNT, HEAD_COUNT * HEAD_SIZE)


def reference(queries, key_rows, value_rows, out_grad, log_decay):
    stacked = (head_major(queries), head_major(key_rows), head_major(value_rows), head_major(out_grad), log_decay.T)
    results = lax.map(lambda items: one_head(items[0], items[1], items[2], items[3], items[4]), stacked)
    return (token_major(results[0]), token_major(results[1]), token_major(results[2]), token_major(results[3]))
```

```python
import functools

import jax
import jax.numpy as jnp
from jax import lax
from jax.experimental import pallas as pl
from jax.experimental.pallas import tpu as pltpu
from jax.sharding import PartitionSpec as P

SIZE = 128
F32 = jnp.float32
BF16 = jnp.bfloat16
MESH = pl.DeviceIdType.MESH


def lower_triangle(rows):
    row = lax.broadcasted_iota(jnp.int32, (rows, rows), 0)
    column = lax.broadcasted_iota(jnp.int32, (rows, rows), 1)
    return row >= column


def over_rows(left, right):
    return lax.dot_general(left, right, (((0,), (0,)), ((), ())), preferred_element_type=F32)


def over_columns(left, right):
    return lax.dot_general(left, right, (((1,), (1,)), ((), ())), preferred_element_type=F32)


def dot(left, right):
    return jnp.dot(left, right, preferred_element_type=F32)


def plan(rounds, parts):
    ready = []
    for i in range(rounds):
        ready.append((11.0 + 1.4 * i, 0.15, "sum", i))
        ready.append((16.2 + 1.4 * i, 0.35, "carry", i))
        ready.append((21.7 + 1.4 * i, 0.3, "pass", i))
        ready.append((22.9 + 1.4 * i, 0.7, "final", i))
    ready.append((9.6, 0.1, "planes", 0))
    ready.sort()
    order, now, part = [], 9.2, 0
    while ready:
        if ready[0][0] > now + 0.1 and part < parts:
            order.append(("inside", part))
            now += 8.6 / parts
            part += 1
            continue
        at, length, step, i = ready.pop(0)
        if step == "final":
            while part < min(parts, -(-parts * (i + 1) // rounds)):
                order.append(("inside", part))
                now += 8.6 / parts
                part += 1
        order.append((step, i))
        now = max(now, at) + length
    return order


def main_kernel(
    planes, devices, q_any, k_any, v_any, g_any, d_any,
    o_ref, dq_ref, dk_ref, dv_ref,
    q_ref, k_ref, v_ref, g_ref, d_ref, decay_rows, forward_rows, backward_rows,
    forward, backward, local, terms, from_core,
    to_chips, from_chips, plane_sum, from_planes, to_back, raw, states,
    own_fin, core_fin, chip_fin, plane_fin,
    load_s, decay_s, fin_s, fin_r, chip_fs, chip_fr, plane_fs, plane_fr,
    core_s, core_r, out_s, out_r, plane_s, plane_r, back_s, back_r, last_s, last_r,
):
    heads, rows = d_any.shape
    chips = devices // 2
    own = heads // chips
    z = lax.axis_index("chain")
    me = lax.axis_index("inner")
    chip, core = me // 2, lax.rem(me, 2)
    kind = 1 - core
    ahead = core == 1

    def place(j):
        return jnp.where(ahead, j, chips - 1 - j)

    def level(j):
        return jnp.where(ahead, j, planes - 1 - j)

    depth = level(z)

    def at_core():
        return (z, chip * 2 + 1 - core)

    def at_chip(other):
        return (z, other * 2 + core)

    def at_plane(other):
        return (other, me)

    def remote(src, dst, send, recv, to):
        return pltpu.make_async_remote_copy(
            src_ref=src, dst_ref=dst, send_sem=send, recv_sem=recv, device_id=to, device_id_type=MESH
        )

    def columns(head):
        return pl.ds(pl.multiple_of(head * SIZE, SIZE), SIZE)

    def loads(i):
        taken = pl.ds(pl.multiple_of(i * (chips * SIZE), SIZE), chips * SIZE)
        pairs = ((k_any, k_ref), (v_any, v_ref), (q_any, q_ref), (g_any, g_ref))
        return [
            pltpu.make_async_copy(src.at[:, taken], dst.at[:, taken], load_s.at[j, i])
            for j, (src, dst) in enumerate(pairs)
        ]

    decay_load = pltpu.make_async_copy(d_any, d_ref, decay_s)
    decay_load.start()

    @pl.loop(0, own)
    def _(i):
        for copy in loads(i):
            copy.start()

    barrier = pltpu.get_barrier_semaphore()
    for step in range(1, planes):
        pl.semaphore_signal(
            barrier, inc=1, device_id=at_plane(lax.rem(z + step, planes)), device_id_type=MESH
        )
    for step in range(1, chips):
        pl.semaphore_signal(
            barrier, inc=1, device_id=at_chip(lax.rem(chip + step, chips)), device_id_type=MESH
        )
    pl.semaphore_signal(barrier, inc=1, device_id=at_core(), device_id_type=MESH)

    lower = lower_triangle(rows)
    row = lax.broadcasted_iota(jnp.int32, (rows, rows), 0)
    column = lax.broadcasted_iota(jnp.int32, (rows, rows), 1)
    upto = (row <= column).astype(F32).astype(BF16)
    after = (row > column).astype(F32).astype(BF16)
    ones = jnp.ones((rows, SIZE), BF16)

    decay_load.wait()
    decay = d_ref[...]
    decay_rows[...] = decay.astype(F32)
    fin = dot(decay, ones)
    cumul = dot(decay, upto)
    own_fin[...] = fin
    forward_rows[...] = jnp.exp(cumul)
    backward_rows[...] = jnp.exp(fin - cumul)

    def make_terms(head):
        taken = columns(head)
        keys = k_ref[:, taken].T.astype(F32) * backward_rows[pl.ds(head, 1), :]
        terms[0, head] = dot(keys.astype(BF16), v_ref[:, taken])
        queries = q_ref[:, taken].T.astype(F32) * forward_rows[pl.ds(head, 1), :]
        terms[1, head] = dot(queries.astype(BF16), g_ref[:, taken])

    @pl.loop(0, own)
    def _(i):
        for copy in loads(i):
            copy.wait()
        for o in range(chips):
            make_terms(i * chips + o)

    def inside(head):
        taken = columns(head)
        query, key, value, grad = (ref[:, taken] for ref in (q_ref, k_ref, v_ref, g_ref))
        picked = jnp.where(lower, decay_rows[pl.ds(head, 1), :], 0.0).astype(BF16)
        spans = dot(picked, jnp.concatenate([after, ones], axis=1))
        weights = jnp.where(lower, jnp.exp(spans[:, :rows]), 0.0)
        sums = spans[:, rows:]
        forward[head] = jnp.exp(sums)
        backward[head] = jnp.exp(own_fin[pl.ds(head, 1), :] - sums)
        probs = (over_columns(query, key) * weights).astype(BF16)
        grows = (over_columns(grad, value) * weights).astype(BF16)
        local[0, head] = dot(probs, value)
        local[1, head] = dot(grows, key)
        local[2, head] = over_rows(grows, query)
        local[3, head] = over_rows(probs, grad)

    pl.semaphore_wait(barrier, chips + planes - 1)

    fin_copy = remote(own_fin, core_fin, fin_s, fin_r, at_core())
    fin_copy.start()

    def core_copy(head):
        return remote(
            terms.at[core, head], from_core.at[head], core_s.at[head], core_r.at[head], at_core()
        )

    @pl.loop(0, heads)
    def _(head):
        core_copy(head).start()

    fin_copy.wait_recv()
    chip_fin[chip] = own_fin[...] + core_fin[...]

    def chip_fin_copy(other, slot):
        return remote(
            chip_fin.at[chip], chip_fin.at[slot], chip_fs.at[other], chip_fr.at[slot], at_chip(other)
        )

    def out_copy(i, other):
        to, slot = i * chips + other, i * chips + chip
        return remote(
            to_chips.at[to], from_chips.at[slot], out_s.at[to], out_r.at[slot], at_chip(other)
        )

    def out_arrival(i, other):
        to = i * chips + other
        return remote(
            to_chips.at[to], from_chips.at[to], out_s.at[to], out_r.at[to], at_chip(other)
        )

    def combine(i):
        for step in range(chips):
            other = lax.rem(chip + 1 + step, chips)
            head = i * chips + other
            core_copy(head).wait_recv()
            factor = jnp.exp(own_fin[pl.ds(head, 1), :])
            total = (terms[kind, head] + factor * from_core[head]).astype(BF16)
            if step < chips - 1:
                to_chips[head] = total
            else:
                from_chips[head] = total
            if step > 0:
                out_copy(i, lax.rem(chip + step, chips)).start()

    combine(0)
    for step in range(1, chips):
        chip_fin_copy(lax.rem(chip + step, chips), chip).start()
    pl.loop(1, own)(combine)

    def plane_fin_copy(other, slot):
        return remote(
            plane_fin.at[z], plane_fin.at[slot], plane_fs.at[other], plane_fr.at[slot],
            at_plane(other),
        )

    def planes_step(_):
        for step in range(1, chips):
            other = lax.rem(chip + step, chips)
            chip_fin_copy(other, other).wait_recv()
        total = chip_fin[0]
        for other in range(1, chips):
            total = total + chip_fin[other]
        plane_fin[z] = total
        for step in range(1, planes):
            plane_fin_copy(lax.rem(z + step, planes), z).start()

    def plane_copy(i, other, slot):
        return remote(
            plane_sum.at[i], from_planes.at[slot, i], plane_s.at[other * own + i],
            plane_r.at[slot * own + i], at_plane(other),
        )

    def factor_of(fins, at, head):
        return jnp.exp(fins[at, pl.ds(head, 1), :])

    def sum_step(i):
        head = i * chips + chip
        for step in range(1, chips):
            out_arrival(i, lax.rem(chip + step, chips)).wait_recv()

        @pl.when(depth < planes - 1)
        def _():
            total = from_chips[i * chips + place(0)].astype(F32)
            for j in range(1, chips):
                at = place(j)
                total = total * factor_of(chip_fin, at, head) + from_chips[i * chips + at].astype(F32)
            plane_sum[i] = total.astype(BF16)

            @pl.loop(0, planes - 1 - depth)
            def _(j):
                plane_copy(i, level(planes - 1 - j), z).start()

    def back_copy(i, other):
        to, slot = i * chips + other, i * chips + chip
        return remote(
            to_back.at[to], raw.at[slot], back_s.at[to], back_r.at[slot], at_chip(other)
        )

    def back_arrival(i, other):
        to = i * chips + other
        return remote(to_back.at[to], raw.at[to], back_s.at[to], back_r.at[to], at_chip(other))

    def carry_step(i):
        head = i * chips + chip
        if i == 0:
            for step in range(1, planes):
                other = lax.rem(z + step, planes)
                plane_fin_copy(other, other).wait_recv()

        def add_plane(j, state):
            at = level(j)
            plane_copy(i, at, at).wait_recv()
            return state * factor_of(plane_fin, at, head) + from_planes[at, i].astype(F32)

        state = lax.fori_loop(0, depth, add_plane, jnp.zeros((SIZE, SIZE), F32))
        for j in range(chips):
            at = place(j)
            to_back[i * chips + at] = state.astype(BF16)
            if j < chips - 1:
                state = state * factor_of(chip_fin, at, head) + from_chips[i * chips + at].astype(F32)
        for step in range(1, chips):
            back_copy(i, lax.rem(chip + step, chips)).start()
        raw[head] = to_back[head]

    def last_copy(head):
        return remote(
            raw.at[head], states.at[kind, head], last_s.at[head], last_r.at[head], at_core()
        )

    def last_arrival(head):
        return remote(
            raw.at[head], states.at[core, head], last_s.at[head], last_r.at[head], at_core()
        )

    def pass_step(i):
        last_copy(i * chips + chip).start()
        for step in range(1, chips):
            other = lax.rem(chip + step, chips)
            back_arrival(i, other).wait_recv()
            last_copy(i * chips + other).start()
        for o in range(chips):
            head = i * chips + o
            factor = jnp.exp(core_fin[pl.ds(head, 1), :])
            states[kind, head] = (factor * raw[head].astype(F32) + from_core[head]).astype(BF16)

    def final_step(i):
        for o in range(chips):
            last_arrival(i * chips + o).wait_recv()
        for o in range(chips):
            head = i * chips + o
            taken = columns(head)
            query, key, value, grad = (ref[:, taken] for ref in (q_ref, k_ref, v_ref, g_ref))
            enter, trail = states[0, head], states[1, head]
            front, behind = forward[head], backward[head]
            o_ref[:, taken] = (local[0, head] + front * dot(query, enter)).astype(BF16)
            dq_ref[:, taken] = (local[1, head] + front * over_columns(grad, enter)).astype(BF16)
            dk_ref[:, taken] = (local[2, head] + behind * over_columns(value, trail)).astype(BF16)
            dv_ref[:, taken] = (local[3, head] + behind * dot(key, trail)).astype(BF16)

    parts = heads // 2

    def inside_step(part):
        for j in range(2):
            inside(part * 2 + j)

    steps = {
        "planes": planes_step, "sum": sum_step, "carry": carry_step, "pass": pass_step,
        "final": final_step, "inside": inside_step,
    }
    for step, i in plan(own, parts):
        steps[step](i)

    fin_copy.wait_send()
    for step in range(1, chips):
        chip_fin_copy(lax.rem(chip + step, chips), chip).wait_send()
    for step in range(1, planes):
        plane_fin_copy(lax.rem(z + step, planes), z).wait_send()

    @pl.loop(0, heads)
    def _(head):
        core_copy(head).wait_send()
        last_copy(head).wait_send()

    @pl.loop(0, own)
    def _(i):
        for step in range(1, chips):
            other = lax.rem(chip + step, chips)
            out_copy(i, other).wait_send()
            back_copy(i, other).wait_send()

        @pl.loop(0, planes - 1 - depth)
        def _(j):
            plane_copy(i, level(planes - 1 - j), z).wait_send()


def computed(planes, devices, arrays):
    decay = pltpu.with_memory_space_constraint(arrays[-1].T, pltpu.HBM)
    arrays = [pltpu.with_memory_space_constraint(item, pltpu.HBM) for item in arrays[:-1]] + [decay]
    heads, rows = decay.shape
    chips = devices // 2
    own = heads // chips
    square = (SIZE, SIZE)
    wide = arrays[0].shape
    dma = pltpu.SemaphoreType.DMA
    return pl.pallas_call(
        functools.partial(main_kernel, planes, devices),
        out_shape=[jax.ShapeDtypeStruct(wide, BF16)] * 4,
        in_specs=[pl.BlockSpec(memory_space=pltpu.HBM)] * 5,
        out_specs=[pl.BlockSpec(memory_space=pltpu.VMEM)] * 4,
        scratch_shapes=[pltpu.VMEM(wide, BF16)] * 4
        + [
            pltpu.VMEM((heads, rows), BF16),
            pltpu.VMEM((heads, rows), F32),
            pltpu.VMEM((heads, rows), F32),
            pltpu.VMEM((heads, rows), F32),
            pltpu.VMEM((heads, rows, SIZE), F32),
            pltpu.VMEM((heads, rows, SIZE), F32),
            pltpu.VMEM((4, heads) + square, F32),
            pltpu.VMEM((2, heads) + square, F32),
            pltpu.VMEM((heads,) + square, F32),
            pltpu.VMEM((heads,) + square, BF16),
            pltpu.VMEM((heads,) + square, BF16),
            pltpu.VMEM((own,) + square, BF16),
            pltpu.VMEM((planes, own) + square, BF16),
            pltpu.VMEM((heads,) + square, BF16),
            pltpu.VMEM((heads,) + square, BF16),
            pltpu.VMEM((2, heads) + square, BF16),
            pltpu.VMEM((heads, SIZE), F32),
            pltpu.VMEM((heads, SIZE), F32),
            pltpu.VMEM((chips, heads, SIZE), F32),
            pltpu.VMEM((planes, heads, SIZE), F32),
            dma((4, own)), dma, dma, dma, dma((chips,)), dma((chips,)), dma((planes,)), dma((planes,)),
            dma((heads,)), dma((heads,)), dma((heads,)), dma((heads,)),
            dma((planes * own,)), dma((planes * own,)),
            dma((heads,)), dma((heads,)), dma((heads,)), dma((heads,)),
        ],
        compiler_params=pltpu.CompilerParams(
            collective_id=0, has_side_effects=True, vmem_limit_bytes=48 * 2**20
        ),
    )(*arrays)


def store_kernel(o_ref, dq_ref, dk_ref, dv_ref, o_out, dq_out, dk_out, dv_out, store_s):
    pairs = ((o_ref, o_out), (dq_ref, dq_out), (dk_ref, dk_out), (dv_ref, dv_out))
    copies = [pltpu.make_async_copy(src, dst, store_s.at[j]) for j, (src, dst) in enumerate(pairs)]
    for copy in copies:
        copy.start()
    for copy in copies:
        copy.wait()


def stored(results):
    return pl.pallas_call(
        store_kernel,
        out_shape=[jax.ShapeDtypeStruct(item.shape, BF16) for item in results],
        in_specs=[pl.BlockSpec(memory_space=pltpu.VMEM)] * 4,
        out_specs=[pl.BlockSpec(memory_space=pltpu.HBM)] * 4,
        scratch_shapes=[pltpu.SemaphoreType.DMA((4,))],
        compiler_params=pltpu.CompilerParams(vmem_limit_bytes=2 * 2**20),
    )(*results)


def solution(mesh):
    planes, devices = mesh.shape["chain"], mesh.shape["inner"]

    def shards(*arrays):
        return tuple(stored(computed(planes, devices, arrays)))

    spec = P(("chain", "inner"), None)
    return jax.shard_map(
        shards, mesh=mesh, in_specs=(spec,) * 5, out_specs=(spec,) * 4, check_vma=False
    )
```

```python
import functools

import jax
import jax.numpy as jnp
from jax import lax
from jax.experimental import pallas as pl
from jax.experimental.pallas import tpu as pltpu
from jax.sharding import PartitionSpec as P

SIZE = 128
F32 = jnp.float32
BF16 = jnp.bfloat16
MESH = pl.DeviceIdType.MESH


def lower_triangle(rows):
    row = lax.broadcasted_iota(jnp.int32, (rows, rows), 0)
    column = lax.broadcasted_iota(jnp.int32, (rows, rows), 1)
    return row >= column


def over_rows(left, right):
    return lax.dot_general(left, right, (((0,), (0,)), ((), ())), preferred_element_type=F32)


def over_columns(left, right):
    return lax.dot_general(left, right, (((1,), (1,)), ((), ())), preferred_element_type=F32)


def dot(left, right):
    return jnp.dot(left, right, preferred_element_type=F32)


def plan(rounds, parts):
    ready = []
    for i in range(rounds):
        ready.append((11.0 + 1.4 * i, 0.15, "sum", i))
        ready.append((16.2 + 1.4 * i, 0.35, "carry", i))
        ready.append((21.7 + 1.4 * i, 0.3, "pass", i))
        ready.append((22.9 + 1.4 * i, 0.7, "final", i))
    ready.append((9.6, 0.1, "planes", 0))
    ready.sort()
    order, now, part = [], 9.2, 0
    while ready:
        if ready[0][0] > now + 0.1 and part < parts:
            order.append(("inside", part))
            now += 8.6 / parts
            part += 1
            continue
        at, length, step, i = ready.pop(0)
        if step == "final":
            while part < min(parts, -(-parts * (i + 1) // rounds)):
                order.append(("inside", part))
                now += 8.6 / parts
                part += 1
        order.append((step, i))
        now = max(now, at) + length
    return order


def main_kernel(
    planes, devices, q_any, k_any, v_any, g_any, d_any,
    o_ref, dq_ref, dk_ref, dv_ref,
    held, d_ref, decay_rows, forward_rows, backward_rows,
    forward, backward, local, terms, from_core,
    to_chips, from_chips, plane_sum, from_planes, to_back, raw, states,
    own_fin, core_fin, chip_fin, plane_fin,
    load_s, decay_s, fin_s, fin_r, chip_fs, chip_fr, plane_fs, plane_fr,
    core_s, first_r, core_r, out_s, out_r, plane_s, plane_r, back_s, back_r, last_s, last_r,
):
    heads, rows = d_any.shape
    chips = devices // 2
    own = heads // chips
    z = lax.axis_index("chain")
    me = lax.axis_index("inner")
    chip, core = me // 2, lax.rem(me, 2)
    kind = 1 - core
    ahead = core == 1

    def place(j):
        return jnp.where(ahead, j, chips - 1 - j)

    def level(j):
        return jnp.where(ahead, j, planes - 1 - j)

    depth = level(z)

    def at_core():
        return (z, chip * 2 + 1 - core)

    def at_chip(other):
        return (z, other * 2 + core)

    def at_plane(other):
        return (other, me)

    def remote(src, dst, send, recv, to):
        return pltpu.make_async_remote_copy(
            src_ref=src, dst_ref=dst, send_sem=send, recv_sem=recv, device_id=to, device_id_type=MESH
        )

    def columns(head):
        return pl.ds(pl.multiple_of(head * SIZE, SIZE), SIZE)

    def loads(i):
        taken = pl.ds(pl.multiple_of(i * (chips * SIZE), SIZE), chips * SIZE)
        return [
            pltpu.make_async_copy(src.at[:, taken], held.at[j, :, taken], load_s.at[i])
            for j, src in enumerate((q_any, k_any, v_any, g_any))
        ]

    def wait_loads(i):
        taken = pl.ds(pl.multiple_of(i * (chips * SIZE), SIZE), chips * SIZE)
        part = held.at[:, :, taken]
        pltpu.make_async_copy(part, part, load_s.at[i]).wait()

    q_ref, k_ref, v_ref, g_ref = (held.at[j] for j in range(4))

    decay_load = pltpu.make_async_copy(d_any, d_ref, decay_s)
    decay_load.start()

    @pl.loop(0, own)
    def _(i):
        for copy in loads(i):
            copy.start()

    barrier = pltpu.get_barrier_semaphore()
    for step in range(1, planes):
        pl.semaphore_signal(
            barrier, inc=1, device_id=at_plane(lax.rem(z + step, planes)), device_id_type=MESH
        )
    for step in range(1, chips):
        pl.semaphore_signal(
            barrier, inc=1, device_id=at_chip(lax.rem(chip + step, chips)), device_id_type=MESH
        )
    pl.semaphore_signal(barrier, inc=1, device_id=at_core(), device_id_type=MESH)

    lower = lower_triangle(rows)
    row = lax.broadcasted_iota(jnp.int32, (rows, rows), 0)
    column = lax.broadcasted_iota(jnp.int32, (rows, rows), 1)
    upto = (row <= column).astype(F32).astype(BF16)
    after = (row > column).astype(F32).astype(BF16)
    ones = jnp.ones((rows, SIZE), BF16)

    decay_load.wait()
    decay = d_ref[...]
    decay_rows[...] = decay.astype(F32)
    fin = dot(decay, ones)
    cumul = dot(decay, upto)
    own_fin[...] = fin
    forward_rows[...] = jnp.exp(cumul)
    backward_rows[...] = jnp.exp(fin - cumul)

    def make_terms(head):
        taken = columns(head)
        keys = k_ref[:, taken].T.astype(F32) * backward_rows[pl.ds(head, 1), :]
        terms[0, head] = dot(keys.astype(BF16), v_ref[:, taken])
        queries = q_ref[:, taken].T.astype(F32) * forward_rows[pl.ds(head, 1), :]
        terms[1, head] = dot(queries.astype(BF16), g_ref[:, taken])

    @pl.loop(0, own)
    def _(i):
        wait_loads(i)
        for o in range(chips):
            make_terms(i * chips + o)

    def inside(head):
        taken = columns(head)
        query, key, value, grad = (ref[:, taken] for ref in (q_ref, k_ref, v_ref, g_ref))
        picked = jnp.where(lower, decay_rows[pl.ds(head, 1), :], 0.0).astype(BF16)
        spans = dot(picked, jnp.concatenate([after, ones], axis=1))
        weights = jnp.where(lower, jnp.exp(spans[:, :rows]), 0.0)
        sums = spans[:, rows:]
        forward[head] = jnp.exp(sums)
        backward[head] = jnp.exp(own_fin[pl.ds(head, 1), :] - sums)
        probs = (over_columns(query, key) * weights).astype(BF16)
        grows = (over_columns(grad, value) * weights).astype(BF16)
        local[0, head] = dot(probs, value)
        local[1, head] = dot(grows, key)
        local[2, head] = over_rows(grows, query)
        local[3, head] = over_rows(probs, grad)

    pl.semaphore_wait(barrier, chips + planes - 1)

    fin_copy = remote(own_fin, core_fin, fin_s, fin_r, at_core())
    fin_copy.start()

    def core_copy(begin, count, recv):
        taken = pl.ds(begin, count)
        return remote(terms.at[core, taken], from_core.at[taken], core_s, recv, at_core())

    def first_copy(o):
        return core_copy(o, 1, first_r.at[o])

    def round_copy(i):
        return core_copy(i * chips, chips, core_r.at[i - 1])

    for step in range(chips):
        first_copy(lax.rem(chip + 1 + step, chips)).start()
    for i in range(1, own):
        round_copy(i).start()

    fin_copy.wait_recv()
    chip_fin[chip] = own_fin[...] + core_fin[...]

    def chip_fin_copy(other, slot):
        return remote(
            chip_fin.at[chip], chip_fin.at[slot], chip_fs, chip_fr, at_chip(other)
        )

    def out_copy(i, other):
        to, slot = i * chips + other, i * chips + chip
        return remote(to_chips.at[to], from_chips.at[slot], out_s, out_r.at[i], at_chip(other))

    def out_copies(count, recv):
        taken = pl.ds(0, count)
        return remote(to_chips.at[taken], from_chips.at[taken], out_s, recv, at_core())

    def combine(i):
        if i > 0:
            round_copy(i).wait_recv()
        for step in range(chips):
            other = lax.rem(chip + 1 + step, chips)
            head = i * chips + other
            if i == 0:
                first_copy(other).wait_recv()
            factor = jnp.exp(own_fin[pl.ds(head, 1), :])
            total = (terms[kind, head] + factor * from_core[head]).astype(BF16)
            if step < chips - 1:
                to_chips[head] = total
            else:
                from_chips[head] = total
            if step > 0:
                out_copy(i, lax.rem(chip + step, chips)).start()

    combine(0)
    for step in range(1, chips):
        chip_fin_copy(lax.rem(chip + step, chips), chip).start()
    for i in range(1, own):
        combine(i)

    def plane_fin_copy(other, slot):
        return remote(
            plane_fin.at[z], plane_fin.at[slot], plane_fs, plane_fr, at_plane(other),
        )

    def planes_step(_):
        taken = chip_fin.at[pl.ds(0, chips - 1)]
        remote(taken, taken, chip_fs, chip_fr, at_core()).wait_recv()
        total = chip_fin[0]
        for other in range(1, chips):
            total = total + chip_fin[other]
        plane_fin[z] = total
        for step in range(1, planes):
            plane_fin_copy(lax.rem(z + step, planes), z).start()

    def plane_copy(i, other, slot):
        return remote(
            plane_sum.at[i], from_planes.at[slot, i], plane_s, plane_r.at[i], at_plane(other)
        )

    def factor_of(fins, at, head):
        return jnp.exp(fins[at, pl.ds(head, 1), :])

    def sum_step(i):
        head = i * chips + chip
        out_copies(chips - 1, out_r.at[i]).wait_recv()

        @pl.when(depth < planes - 1)
        def _():
            total = from_chips[i * chips + place(0)].astype(F32)
            for j in range(1, chips):
                at = place(j)
                total = total * factor_of(chip_fin, at, head) + from_chips[i * chips + at].astype(F32)
            plane_sum[i] = total.astype(BF16)

            @pl.loop(0, planes - 1 - depth)
            def _(j):
                plane_copy(i, level(planes - 1 - j), z).start()

    def back_copy(i, other):
        to, slot = i * chips + other, i * chips + chip
        return remote(to_back.at[to], raw.at[slot], back_s, back_r.at[i], at_chip(other))

    def back_copies(count, recv):
        taken = pl.ds(0, count)
        return remote(to_back.at[taken], raw.at[taken], back_s, recv, at_core())

    def carry_step(i):
        head = i * chips + chip
        if i == 0:
            taken = plane_fin.at[pl.ds(0, planes - 1)]
            remote(taken, taken, plane_fs, plane_fr, at_core()).wait_recv()
        for count in range(1, planes):
            @pl.when(depth == count)
            def _():
                taken = from_planes.at[pl.ds(0, count), i]
                remote(taken, taken, plane_s, plane_r.at[i], at_core()).wait_recv()

        def add_plane(j, state):
            at = level(j)
            return state * factor_of(plane_fin, at, head) + from_planes[at, i].astype(F32)

        state = lax.fori_loop(0, depth, add_plane, jnp.zeros((SIZE, SIZE), F32))
        for j in range(chips):
            at = place(j)
            to_back[i * chips + at] = state.astype(BF16)
            if j < chips - 1:
                state = state * factor_of(chip_fin, at, head) + from_chips[i * chips + at].astype(F32)
        for step in range(1, chips):
            back_copy(i, lax.rem(chip + step, chips)).start()
        raw[head] = to_back[head]

    def last_copy(i):
        taken = pl.ds(i * chips, chips)
        return remote(raw.at[taken], states.at[kind, taken], last_s, last_r.at[i], at_core())

    def pass_step(i):
        back_copies(chips - 1, back_r.at[i]).wait_recv()
        last_copy(i).start()
        for o in range(chips):
            head = i * chips + o
            factor = jnp.exp(core_fin[pl.ds(head, 1), :])
            states[kind, head] = (factor * raw[head].astype(F32) + from_core[head]).astype(BF16)

    def final_step(i):
        last_copy(i).wait_recv()
        for o in range(chips):
            head = i * chips + o
            taken = columns(head)
            query, key, value, grad = (ref[:, taken] for ref in (q_ref, k_ref, v_ref, g_ref))
            enter, trail = states[0, head], states[1, head]
            front, behind = forward[head], backward[head]
            o_ref[:, taken] = (local[0, head] + front * dot(query, enter)).astype(BF16)
            dq_ref[:, taken] = (local[1, head] + front * over_columns(grad, enter)).astype(BF16)
            dk_ref[:, taken] = (local[2, head] + behind * over_columns(value, trail)).astype(BF16)
            dv_ref[:, taken] = (local[3, head] + behind * dot(key, trail)).astype(BF16)

    parts = heads // 2

    def inside_step(part):
        for j in range(2):
            inside(part * 2 + j)

    steps = {
        "planes": planes_step, "sum": sum_step, "carry": carry_step, "pass": pass_step,
        "final": final_step, "inside": inside_step,
    }
    for step, i in plan(own, parts):
        steps[step](i)

    fin_copy.wait_send()
    taken = chip_fin.at[pl.ds(0, chips - 1)]
    remote(taken, taken, chip_fs, chip_fr, at_core()).wait_send()
    taken = plane_fin.at[pl.ds(0, planes - 1)]
    remote(taken, taken, plane_fs, plane_fr, at_core()).wait_send()
    core_copy(0, heads, core_r.at[0]).wait_send()
    out_copies(own * (chips - 1), out_r.at[0]).wait_send()
    back_copies(own * (chips - 1), back_r.at[0]).wait_send()
    remote(raw, states.at[kind], last_s, last_r.at[0], at_core()).wait_send()
    for count in range(1, planes):
        @pl.when(planes - 1 - depth == count)
        def _():
            taken = from_planes.at[pl.ds(0, count)]
            remote(taken, taken, plane_s, plane_r.at[0], at_core()).wait_send()


def computed(planes, devices, arrays):
    decay = pltpu.with_memory_space_constraint(arrays[-1].T, pltpu.HBM)
    arrays = [pltpu.with_memory_space_constraint(item, pltpu.HBM) for item in arrays[:-1]] + [decay]
    heads, rows = decay.shape
    chips = devices // 2
    own = heads // chips
    square = (SIZE, SIZE)
    wide = arrays[0].shape
    dma = pltpu.SemaphoreType.DMA
    return pl.pallas_call(
        functools.partial(main_kernel, planes, devices),
        out_shape=[jax.ShapeDtypeStruct(wide, BF16)] * 4,
        in_specs=[pl.BlockSpec(memory_space=pltpu.HBM)] * 5,
        out_specs=[pl.BlockSpec(memory_space=pltpu.VMEM)] * 4,
        scratch_shapes=[
            pltpu.VMEM((4,) + wide, BF16),
            pltpu.VMEM((heads, rows), BF16),
            pltpu.VMEM((heads, rows), F32),
            pltpu.VMEM((heads, rows), F32),
            pltpu.VMEM((heads, rows), F32),
            pltpu.VMEM((heads, rows, SIZE), F32),
            pltpu.VMEM((heads, rows, SIZE), F32),
            pltpu.VMEM((4, heads) + square, F32),
            pltpu.VMEM((2, heads) + square, F32),
            pltpu.VMEM((heads,) + square, F32),
            pltpu.VMEM((heads,) + square, BF16),
            pltpu.VMEM((heads,) + square, BF16),
            pltpu.VMEM((own,) + square, BF16),
            pltpu.VMEM((planes, own) + square, BF16),
            pltpu.VMEM((heads,) + square, BF16),
            pltpu.VMEM((heads,) + square, BF16),
            pltpu.VMEM((2, heads) + square, BF16),
            pltpu.VMEM((heads, SIZE), F32),
            pltpu.VMEM((heads, SIZE), F32),
            pltpu.VMEM((chips, heads, SIZE), F32),
            pltpu.VMEM((planes, heads, SIZE), F32),
            dma((own,)), dma, dma, dma, dma, dma, dma, dma,
            dma, dma((chips,)), dma((own,)), dma, dma((own,)), dma, dma((own,)),
            dma, dma((own,)), dma, dma((own,)),
        ],
        compiler_params=pltpu.CompilerParams(
            collective_id=0, has_side_effects=True, vmem_limit_bytes=48 * 2**20
        ),
    )(*arrays)


def store_kernel(o_ref, dq_ref, dk_ref, dv_ref, o_out, dq_out, dk_out, dv_out, store_s):
    pairs = ((o_ref, o_out), (dq_ref, dq_out), (dk_ref, dk_out), (dv_ref, dv_out))
    copies = [pltpu.make_async_copy(src, dst, store_s.at[j]) for j, (src, dst) in enumerate(pairs)]
    for copy in copies:
        copy.start()
    for copy in copies:
        copy.wait()


def stored(results):
    return pl.pallas_call(
        store_kernel,
        out_shape=[jax.ShapeDtypeStruct(item.shape, BF16) for item in results],
        in_specs=[pl.BlockSpec(memory_space=pltpu.VMEM)] * 4,
        out_specs=[pl.BlockSpec(memory_space=pltpu.HBM)] * 4,
        scratch_shapes=[pltpu.SemaphoreType.DMA((4,))],
        compiler_params=pltpu.CompilerParams(vmem_limit_bytes=2 * 2**20),
    )(*results)


def solution(mesh):
    planes, devices = mesh.shape["chain"], mesh.shape["inner"]

    def shards(*arrays):
        return tuple(stored(computed(planes, devices, arrays)))

    spec = P(("chain", "inner"), None)
    return jax.shard_map(
        shards, mesh=mesh, in_specs=(spec,) * 5, out_specs=(spec,) * 4, check_vma=False
    )
```

```python
import functools

import jax
import jax.numpy as jnp
from jax import lax
from jax.experimental import pallas as pl
from jax.experimental.pallas import tpu as pltpu
from jax.sharding import PartitionSpec as P

SIZE = 128
F32 = jnp.float32
BF16 = jnp.bfloat16
MESH = pl.DeviceIdType.MESH


def lower_triangle(rows):
    row = lax.broadcasted_iota(jnp.int32, (rows, rows), 0)
    column = lax.broadcasted_iota(jnp.int32, (rows, rows), 1)
    return row >= column


def over_rows(left, right):
    return lax.dot_general(left, right, (((0,), (0,)), ((), ())), preferred_element_type=F32)


def over_columns(left, right):
    return lax.dot_general(left, right, (((1,), (1,)), ((), ())), preferred_element_type=F32)


def dot(left, right):
    return jnp.dot(left, right, preferred_element_type=F32)


def plan(rounds, parts):
    ready = []
    for i in range(rounds):
        ready.append((9.0 + 1.4 * i, 0.15, "sum", i))
        ready.append((14.0 + 1.4 * i, 0.35, "carry", i))
        ready.append((19.7 + 1.4 * i, 0.6, "pass", i))
        ready.append((21.1 + 1.4 * i, 0.35, "other", i))
    ready.append((8.4, 0.1, "planes", 0))
    ready.sort()
    order, now, part = [], 7.6, 0
    while ready:
        if ready[0][0] > now + 0.1 and part < parts:
            order.append(("inside", part))
            now += 8.6 / parts
            part += 1
            continue
        at, length, step, i = ready.pop(0)
        if step == "pass":
            while part < min(parts, -(-parts * (i + 1) // rounds)):
                order.append(("inside", part))
                now += 8.6 / parts
                part += 1
        order.append((step, i))
        now = max(now, at) + length
    return order


def main_kernel(
    planes, devices, q_any, k_any, v_any, g_any, d_any, out_ref,
    held, d_ref, decay_rows, forward_rows, backward_rows,
    scales, local, terms, from_core,
    to_chips, from_chips, plane_sum, from_planes, to_back, raw, states,
    own_fin, core_fin, chip_total, chip_fin, plane_fin,
    load_s, decay_s, go_s, fin_s, fin_r, chip_fs, chip_fr, plane_fs, plane_fr,
    core_s, core_r, out_s, out_r, plane_s, plane_r, back_s, back_r, last_s, last_r,
):
    heads, rows = d_any.shape
    chips = devices // 2
    own = heads // chips
    z = lax.axis_index("chain")
    me = lax.axis_index("inner")
    chip, core = me // 2, lax.rem(me, 2)
    kind = 1 - core
    ahead = core == 1

    def place(j):
        return jnp.where(ahead, j, chips - 1 - j)

    def level(j):
        return jnp.where(ahead, j, planes - 1 - j)

    depth, spot = level(z), place(chip)
    first = (depth == 0) & (spot == 0)
    last = (depth == planes - 1) & (spot == chips - 1)

    def partner(m):
        if chips & (chips - 1):
            return lax.rem(chip + m, chips)
        bits = [(1 << b, (m >> b) & 1) for b in range(chips.bit_length() - 1)]
        return sum(lax.rem(chip // size + bit, 2) * size for size, bit in bits)

    hops = sorted(range(1, chips), key=lambda m: -bin(m).count("1"))

    def at_core():
        return (z, chip * 2 + 1 - core)

    def at_chip(other):
        return (z, other * 2 + core)

    def at_plane(other):
        return (other, me)

    def remote(src, dst, send, recv, to):
        return pltpu.make_async_remote_copy(
            src_ref=src, dst_ref=dst, send_sem=send, recv_sem=recv, device_id=to, device_id_type=MESH
        )

    def columns(head):
        return pl.ds(pl.multiple_of(head * SIZE, SIZE), SIZE)

    def round_columns(i):
        return pl.ds(pl.multiple_of(i * (chips * SIZE), SIZE), chips * SIZE)

    decay_load = pltpu.make_async_copy(d_any, d_ref, decay_s)
    decay_load.start()

    @pl.loop(0, own)
    def _(i):
        taken = round_columns(i)
        for j, src in enumerate((q_any, k_any, g_any, v_any)):
            pltpu.make_async_copy(src.at[:, taken], held.at[j, :, taken], load_s.at[i]).start()

    barrier = pltpu.get_barrier_semaphore()

    def greet(to):
        pl.semaphore_signal(barrier, inc=1, device_id=to, device_id_type=MESH)

    for step in range(1, planes):
        greet((lax.rem(z + step, planes), chip * 2 + 1))
    for m in hops:
        greet((z, partner(m) * 2 + 1))
    greet(at_core())

    lower = lower_triangle(rows)
    row = lax.broadcasted_iota(jnp.int32, (rows, rows), 0)
    column = lax.broadcasted_iota(jnp.int32, (rows, rows), 1)
    upto = (row <= column).astype(F32).astype(BF16)
    after = (row > column).astype(F32).astype(BF16)
    ones = jnp.ones((rows, SIZE), BF16)
    row = lax.broadcasted_iota(jnp.int32, (heads, heads), 0)
    column = lax.broadcasted_iota(jnp.int32, (heads, heads), 1)
    owners = (column == (row % own) * chips + row // own).astype(F32).astype(BF16)

    decay_load.wait()
    decay = d_ref[...]
    decay_rows[...] = decay.astype(F32)
    by_owner = dot(dot(owners, decay).astype(BF16), ones)
    for o in range(chips):
        own_fin[o] = by_owner[o * own : (o + 1) * own]
    fin = dot(decay, ones)
    cumul = dot(decay, upto)
    forward_rows[...] = jnp.exp(cumul)
    backward_rows[...] = jnp.exp(fin - cumul)

    fin_copy = remote(own_fin, core_fin, fin_s, fin_r, at_core())

    def core_copies(begin, count, recv):
        taken = pl.ds(begin, count)
        return remote(terms.at[core, taken], from_core.at[taken], core_s, recv, at_core())

    def core_copy(i):
        return core_copies(i * chips, chips, core_r.at[i])

    @pl.when(core == 0)
    def _():
        pl.semaphore_wait(barrier, 1)
        fin_copy.start()

    def make_terms(head):
        taken = columns(head)
        keys = held[1, :, taken].T.astype(F32) * backward_rows[pl.ds(head, 1), :]
        terms[0, head] = dot(keys.astype(BF16), held[3, :, taken])
        queries = held[0, :, taken].T.astype(F32) * forward_rows[pl.ds(head, 1), :]
        terms[1, head] = dot(queries.astype(BF16), held[2, :, taken])

    @pl.loop(0, own)
    def _(i):
        part = held.at[:, :, round_columns(i)]
        pltpu.make_async_copy(part, part, load_s.at[i]).wait()
        for o in range(chips):
            make_terms(i * chips + o)

        @pl.when(core == 0)
        def _():
            core_copy(i).start()

    @pl.when(core == 1)
    def _():
        pl.semaphore_wait(barrier, 2 * (chips + planes) - 3)
        pl.semaphore_signal(go_s, inc=1, device_id=at_core(), device_id_type=MESH)
        fin_copy.start()
        for i in range(own):
            core_copy(i).start()

    @pl.when(core == 0)
    def _():
        pl.semaphore_wait(go_s, 1)

    def inside(head):
        taken = columns(head)
        query, key, grad, value = (held[j, :, taken] for j in range(4))
        picked = jnp.where(lower, decay_rows[pl.ds(head, 1), :], 0.0).astype(BF16)
        spans = dot(picked, jnp.concatenate([after, ones], axis=1))
        weights = jnp.where(lower, jnp.exp(spans[:, :rows]), 0.0)
        sums = spans[:, rows:]
        scales[0, head] = jnp.exp(sums)
        scales[1, head] = jnp.exp(own_fin[lax.rem(head, chips), pl.ds(head // chips, 1), :] - sums)
        probs = (over_columns(query, key) * weights).astype(BF16)
        grows = (over_columns(grad, value) * weights).astype(BF16)
        local[0, head] = dot(probs, value)
        local[1, head] = over_rows(probs, grad)
        local[2, head] = dot(grows, key)
        local[3, head] = over_rows(grows, query)

    def chip_fin_copy(other):
        return remote(
            chip_total.at[other], chip_fin.at[chip], chip_fs, chip_fr, at_chip(other)
        )

    def out_copy(i, other):
        to, slot = i * chips + other, i * chips + chip
        return remote(to_chips.at[to], from_chips.at[slot], out_s, out_r.at[i], at_chip(other))

    def out_copies(count, recv):
        taken = pl.ds(0, count)
        return remote(to_chips.at[taken], from_chips.at[taken], out_s, recv, at_core())

    def combine(i):
        core_copy(i).wait_recv()
        waiting = None
        for m in hops + [0]:
            other = partner(m) if m else chip
            head = i * chips + other
            factor = jnp.exp(own_fin[other, pl.ds(i, 1), :])
            total = (terms[kind, head] + factor * from_core[head]).astype(BF16)
            if m:
                to_chips[head] = total
            else:
                from_chips[head] = total
            if waiting is not None:
                @pl.when(jnp.logical_not(last))
                def _():
                    out_copy(i, waiting).start()
            waiting = other

    combine(0)
    fin_copy.wait_recv()
    chip_total[...] = own_fin[...] + core_fin[...]
    if own > 1:
        combine(1)
    chip_fin[chip] = chip_total[chip]
    for m in hops:
        chip_fin_copy(partner(m)).start()
    for i in range(2, own):
        combine(i)

    def plane_fin_copy(other):
        return remote(plane_fin.at[z], plane_fin.at[z], plane_fs, plane_fr, at_plane(other))

    def planes_step(_):
        taken = chip_fin.at[pl.ds(0, chips - 1)]
        remote(taken, taken, chip_fs, chip_fr, at_core()).wait_recv()
        total = chip_fin[0]
        for other in range(1, chips):
            total = total + chip_fin[other]
        plane_fin[z] = total
        for step in range(1, planes):
            plane_fin_copy(lax.rem(z + step, planes)).start()

    def plane_copy(i, other):
        return remote(
            plane_sum.at[i], from_planes.at[z, i], plane_s, plane_r.at[i], at_plane(other)
        )

    def factor_of(fins, at, i):
        return jnp.exp(fins[at, pl.ds(i, 1), :])

    def sum_step(i):
        fewer = (depth == planes - 1) & (spot < chips - 1)
        for few, count in ((fewer, chips - 2), (jnp.logical_not(fewer), chips - 1)):
            @pl.when(few)
            def _():
                out_copies(count, out_r.at[i]).wait_recv()

        @pl.when(depth < planes - 1)
        def _():
            total = from_chips[i * chips + place(0)].astype(F32)
            for j in range(1, chips):
                at = place(j)
                total = total * factor_of(chip_fin, at, i) + from_chips[i * chips + at].astype(F32)
            plane_sum[i] = total.astype(BF16)

            @pl.loop(0, planes - 1 - depth)
            def _(j):
                plane_copy(i, level(planes - 1 - j)).start()

    def back_copy(i, other):
        to, slot = i * chips + other, i * chips + chip
        return remote(to_back.at[to], raw.at[slot], back_s, back_r.at[i], at_chip(other))

    def back_copies(count, recv):
        taken = pl.ds(0, count)
        return remote(to_back.at[taken], raw.at[taken], back_s, recv, at_core())

    def carry_step(i):
        head = i * chips + chip
        if i == 0:
            taken = plane_fin.at[pl.ds(0, planes - 1)]
            remote(taken, taken, plane_fs, plane_fr, at_core()).wait_recv()
        for count in range(1, planes):
            @pl.when(depth == count)
            def _():
                taken = from_planes.at[pl.ds(0, count), i]
                remote(taken, taken, plane_s, plane_r.at[i], at_core()).wait_recv()

        def add_plane(j, state):
            at = level(j)
            return state * factor_of(plane_fin, at, i) + from_planes[at, i].astype(F32)

        state = lax.fori_loop(0, depth, add_plane, jnp.zeros((SIZE, SIZE), F32))
        for j in range(chips):
            at = place(j)
            to_back[i * chips + at] = state.astype(BF16)
            if j < chips - 1:
                state = state * factor_of(chip_fin, at, i) + from_chips[i * chips + at].astype(F32)
        for m in hops:
            other = partner(m)

            @pl.when((depth > 0) | (other != place(0)))
            def _():
                back_copy(i, other).start()
        raw[head] = to_back[head]

    def last_copy(i):
        taken = pl.ds(i * chips, chips)
        return remote(raw.at[taken], states.at[taken], last_s, last_r.at[i], at_core())

    def apply(which, head, state):
        taken = columns(head)
        scale = scales[which, head]
        straight = dot(held[which, :, taken], state)
        out_ref[which, :, taken] = (local[which, head] + scale * straight).astype(BF16)
        turned = over_columns(held[2 + which, :, taken], state)
        out_ref[2 + which, :, taken] = (local[2 + which, head] + scale * turned).astype(BF16)

    def pass_step(i):
        @pl.when(jnp.logical_not(first))
        def _():
            back_copies(chips - 1, back_r.at[i]).wait_recv()
        last_copy(i).start()
        for o in range(chips):
            head = i * chips + o
            factor = jnp.exp(core_fin[o, pl.ds(i, 1), :])
            apply(kind, head, (factor * raw[head].astype(F32) + from_core[head]).astype(BF16))

    def other_step(i):
        last_copy(i).wait_recv()
        for o in range(chips):
            head = i * chips + o
            apply(core, head, states[head])

    @pl.when(first)
    def _():
        @pl.loop(0, heads)
        def _(head):
            raw[head] = jnp.zeros((SIZE, SIZE), BF16)

    parts = heads // 2

    def inside_step(part):
        for j in range(2):
            inside(part * 2 + j)

    steps = {
        "planes": planes_step, "sum": sum_step, "carry": carry_step, "pass": pass_step,
        "other": other_step, "inside": inside_step,
    }
    for step, i in plan(own, parts):
        steps[step](i)

    fin_copy.wait_send()
    taken = chip_fin.at[pl.ds(0, chips - 1)]
    remote(taken, taken, chip_fs, chip_fr, at_core()).wait_send()
    taken = plane_fin.at[pl.ds(0, planes - 1)]
    remote(taken, taken, plane_fs, plane_fr, at_core()).wait_send()
    core_copies(0, heads, core_r.at[0]).wait_send()

    @pl.when(jnp.logical_not(last))
    def _():
        out_copies(own * (chips - 1), out_r.at[0]).wait_send()
    fewer = (depth == 0) & (spot > 0)
    for few, count in ((fewer, chips - 2), (jnp.logical_not(fewer), chips - 1)):
        @pl.when(few)
        def _():
            back_copies(own * count, back_r.at[0]).wait_send()
    remote(raw, states, last_s, last_r.at[0], at_core()).wait_send()
    for count in range(1, planes):
        @pl.when(planes - 1 - depth == count)
        def _():
            taken = from_planes.at[pl.ds(0, count)]
            remote(taken, taken, plane_s, plane_r.at[0], at_core()).wait_send()


def computed(planes, devices, arrays):
    decay = pltpu.with_memory_space_constraint(arrays[-1].T, pltpu.HBM)
    arrays = [pltpu.with_memory_space_constraint(item, pltpu.HBM) for item in arrays[:-1]] + [decay]
    heads, rows = decay.shape
    chips = devices // 2
    own = heads // chips
    square = (SIZE, SIZE)
    wide = arrays[0].shape
    dma = pltpu.SemaphoreType.DMA
    return pl.pallas_call(
        functools.partial(main_kernel, planes, devices),
        out_shape=jax.ShapeDtypeStruct((4,) + wide, BF16),
        in_specs=[pl.BlockSpec(memory_space=pltpu.HBM)] * 5,
        out_specs=pl.BlockSpec(memory_space=pltpu.VMEM),
        scratch_shapes=[
            pltpu.VMEM((4,) + wide, BF16),
            pltpu.VMEM((heads, rows), BF16),
            pltpu.VMEM((heads, rows), F32),
            pltpu.VMEM((heads, rows), F32),
            pltpu.VMEM((heads, rows), F32),
            pltpu.VMEM((2, heads, rows, SIZE), F32),
            pltpu.VMEM((4, heads) + square, F32),
            pltpu.VMEM((2, heads) + square, F32),
            pltpu.VMEM((heads,) + square, F32),
            pltpu.VMEM((heads,) + square, BF16),
            pltpu.VMEM((heads,) + square, BF16),
            pltpu.VMEM((own,) + square, BF16),
            pltpu.VMEM((planes, own) + square, BF16),
            pltpu.VMEM((heads,) + square, BF16),
            pltpu.VMEM((heads,) + square, BF16),
            pltpu.VMEM((heads,) + square, BF16),
            pltpu.VMEM((chips, own, SIZE), F32),
            pltpu.VMEM((chips, own, SIZE), F32),
            pltpu.VMEM((chips, own, SIZE), F32),
            pltpu.VMEM((chips, own, SIZE), F32),
            pltpu.VMEM((planes, own, SIZE), F32),
            dma((own,)), dma, pltpu.SemaphoreType.REGULAR, dma, dma, dma, dma, dma, dma,
            dma, dma((own,)), dma, dma((own,)), dma, dma((own,)),
            dma, dma((own,)), dma, dma((own,)),
        ],
        compiler_params=pltpu.CompilerParams(
            collective_id=0, has_side_effects=True, vmem_limit_bytes=48 * 2**20
        ),
    )(*arrays)


def store_kernel(held, o_out, dq_out, dk_out, dv_out, store_s):
    copies = [
        pltpu.make_async_copy(held.at[j], dst, store_s.at[j])
        for j, dst in enumerate((o_out, dv_out, dq_out, dk_out))
    ]
    for copy in copies:
        copy.start()
    for copy in copies:
        copy.wait()


def stored(results):
    return pl.pallas_call(
        store_kernel,
        out_shape=[jax.ShapeDtypeStruct(results.shape[1:], BF16)] * 4,
        in_specs=[pl.BlockSpec(memory_space=pltpu.VMEM)],
        out_specs=[pl.BlockSpec(memory_space=pltpu.HBM)] * 4,
        scratch_shapes=[pltpu.SemaphoreType.DMA((4,))],
        compiler_params=pltpu.CompilerParams(vmem_limit_bytes=2 * 2**20),
    )(results)


def solution(mesh):
    planes, devices = mesh.shape["chain"], mesh.shape["inner"]

    def shards(*arrays):
        return tuple(stored(computed(planes, devices, arrays)))

    spec = P(("chain", "inner"), None)
    return jax.shard_map(
        shards, mesh=mesh, in_specs=(spec,) * 5, out_specs=(spec,) * 4, check_vma=False
    )
```

```python
import functools

import jax
import jax.numpy as jnp
from jax import lax
from jax.experimental import pallas as pl
from jax.experimental.pallas import tpu as pltpu
from jax.sharding import PartitionSpec as P

SIZE = 128
F32 = jnp.float32
BF16 = jnp.bfloat16
MESH = pl.DeviceIdType.MESH


def lower_triangle(rows):
    row = lax.broadcasted_iota(jnp.int32, (rows, rows), 0)
    column = lax.broadcasted_iota(jnp.int32, (rows, rows), 1)
    return row >= column


def over_rows(left, right):
    return lax.dot_general(left, right, (((0,), (0,)), ((), ())), preferred_element_type=F32)


def over_columns(left, right):
    return lax.dot_general(left, right, (((1,), (1,)), ((), ())), preferred_element_type=F32)


def dot(left, right):
    return jnp.dot(left, right, preferred_element_type=F32)


def plan(ready, rounds, parts, now):
    ready = sorted(ready)
    order, part = [], 0
    while ready:
        if ready[0][0] > now + 0.1 and part < parts:
            order.append(("inside", part))
            now += 8.6 / parts
            part += 1
            continue
        at, length, step, i = ready.pop(0)
        if step in ("pass", "other"):
            while part < min(parts, -(-parts * (i + 1) // rounds)):
                order.append(("inside", part))
                now += 8.6 / parts
                part += 1
        order.append((step, i))
        now = max(now, at) + length
    return order


def lead_plan(rounds, parts):
    ready = [(7.5, 0.1, "planes", 0)]
    for i in range(rounds):
        ready.append((7.8 + 0.7 * i, 0.15, "sum", i))
        ready.append((14.0 + 0.7 * i, 0.35, "carry", i))
        ready.append((19.0 + 0.7 * i, 0.55, "pass", i))
        ready.append((25.7 + 0.7 * i, 0.35, "other", i))
    turn = min(2, rounds - 1)
    ready.append((7.81 + 0.7 * turn, 0.01, "turn", 0))
    return plan(ready, rounds, parts, 6.7)


def tail_plan(rounds, parts):
    ready = [(9.5, 0.1, "turn", 0), (13.3, 0.05, "share", 0)]
    for i in range(rounds):
        ready.append((5.1 + 0.3 * i, 0.3, "combine", i))
        ready.append((13.4 + 0.7 * i, 0.15, "sum", i))
        ready.append((17.5 + 0.7 * i, 0.35, "carry", i))
        ready.append((24.6 + 0.7 * i, 0.55, "pass", i))
        ready.append((20.1 + 0.7 * i, 0.35, "other", i))
    return plan(ready, rounds, parts, 4.5)


def main_kernel(
    planes, devices, q_any, k_any, v_any, g_any, d_any, out_ref,
    held, d_ref, decay_rows, forward_rows, backward_rows,
    scales, local, terms, from_core,
    to_chips, from_chips, plane_sum, from_planes, to_back, raw, states,
    own_fin, core_fin, chip_total, chip_fin, plane_fin,
    load_s, decay_s, go_s, fin_s, fin_r, chip_fs, chip_fr, plane_fs, plane_fr, share_s, share_r,
    core_s, core_r, out_s, out_r, plane_s, plane_r, back_s, back_r, last_s, last_r,
):
    heads, rows = d_any.shape
    chips = devices // 2
    own = heads // chips
    z = lax.axis_index("chain")
    me = lax.axis_index("inner")
    chip, core = me // 2, lax.rem(me, 2)
    kind = 1 - core
    ahead = core == 1

    def place(j):
        return jnp.where(ahead, j, chips - 1 - j)

    def level(j):
        return jnp.where(ahead, j, planes - 1 - j)

    depth, spot = level(z), place(chip)

    def lead_core(plane):
        return jnp.where(plane * 2 < planes, 1, 0)

    lead = core == lead_core(z)
    first = (depth == 0) & (spot == 0)
    last = (depth == planes - 1) & (spot == chips - 1)

    def partner(m):
        if chips & (chips - 1):
            return lax.rem(chip + m, chips)
        bits = [(1 << b, (m >> b) & 1) for b in range(chips.bit_length() - 1)]
        return sum(lax.rem(chip // size + bit, 2) * size for size, bit in bits)

    hops = sorted(range(1, chips), key=lambda m: -bin(m).count("1"))

    def at_core():
        return (z, chip * 2 + 1 - core)

    def at_chip(other):
        return (z, other * 2 + core)

    def at_plane(other):
        return (other, me)

    def remote(src, dst, send, recv, to):
        return pltpu.make_async_remote_copy(
            src_ref=src, dst_ref=dst, send_sem=send, recv_sem=recv, device_id=to, device_id_type=MESH
        )

    def columns(head):
        return pl.ds(pl.multiple_of(head * SIZE, SIZE), SIZE)

    def round_columns(i):
        return pl.ds(pl.multiple_of(i * (chips * SIZE), SIZE), chips * SIZE)

    decay_load = pltpu.make_async_copy(d_any, d_ref, decay_s)
    decay_load.start()

    @pl.loop(0, own)
    def _(i):
        taken = round_columns(i)
        for j, src in enumerate((q_any, k_any, g_any, v_any)):
            pltpu.make_async_copy(src.at[:, taken], held.at[j, :, taken], load_s.at[i]).start()

    barrier = pltpu.get_barrier_semaphore()

    def greet(to):
        pl.semaphore_signal(barrier, inc=1, device_id=to, device_id_type=MESH)

    for step in range(1, planes):
        plane = lax.rem(z + step, planes)
        greet((plane, chip * 2 + lead_core(plane)))
    for m in hops:
        greet((z, partner(m) * 2 + lead_core(z)))
    greet(at_core())

    lower = lower_triangle(rows)
    row = lax.broadcasted_iota(jnp.int32, (rows, rows), 0)
    column = lax.broadcasted_iota(jnp.int32, (rows, rows), 1)
    upto = (row <= column).astype(F32).astype(BF16)
    after = (row > column).astype(F32).astype(BF16)
    ones = jnp.ones((rows, SIZE), BF16)
    row = lax.broadcasted_iota(jnp.int32, (heads, heads), 0)
    column = lax.broadcasted_iota(jnp.int32, (heads, heads), 1)
    owners = (column == (row % own) * chips + row // own).astype(F32).astype(BF16)

    decay_load.wait()
    decay = d_ref[...]
    decay_rows[...] = decay.astype(F32)
    by_owner = dot(dot(owners, decay).astype(BF16), ones)
    for o in range(chips):
        own_fin[o] = by_owner[o * own : (o + 1) * own]
    fin = dot(decay, ones)
    cumul = dot(decay, upto)
    forward_rows[...] = jnp.exp(cumul)
    backward_rows[...] = jnp.exp(fin - cumul)

    fin_copy = remote(own_fin, core_fin, fin_s, fin_r, at_core())

    def core_copies(begin, count, recv):
        taken = pl.ds(begin, count)
        return remote(terms.at[core, taken], from_core.at[taken], core_s, recv, at_core())

    def core_copy(i):
        return core_copies(i * chips, chips, core_r.at[i])

    def make_terms(head):
        taken = columns(head)
        keys = held[1, :, taken].T.astype(F32) * backward_rows[pl.ds(head, 1), :]
        terms[0, head] = dot(keys.astype(BF16), held[3, :, taken])
        queries = held[0, :, taken].T.astype(F32) * forward_rows[pl.ds(head, 1), :]
        terms[1, head] = dot(queries.astype(BF16), held[2, :, taken])

    def terms_step(i):
        part = held.at[:, :, round_columns(i)]
        pltpu.make_async_copy(part, part, load_s.at[i]).wait()
        for o in range(chips):
            make_terms(i * chips + o)

    def inside(head):
        taken = columns(head)
        query, key, grad, value = (held[j, :, taken] for j in range(4))
        picked = jnp.where(lower, decay_rows[pl.ds(head, 1), :], 0.0).astype(BF16)
        spans = dot(picked, jnp.concatenate([after, ones], axis=1))
        weights = jnp.where(lower, jnp.exp(spans[:, :rows]), 0.0)
        sums = spans[:, rows:]
        scales[0, head] = jnp.exp(sums)
        scales[1, head] = jnp.exp(own_fin[lax.rem(head, chips), pl.ds(head // chips, 1), :] - sums)
        probs = (over_columns(query, key) * weights).astype(BF16)
        grows = (over_columns(grad, value) * weights).astype(BF16)
        local[0, head] = dot(probs, value)
        local[1, head] = over_rows(probs, grad)
        local[2, head] = dot(grows, key)
        local[3, head] = over_rows(grows, query)

    def chip_fin_copy(other):
        return remote(
            chip_total.at[other], chip_fin.at[chip], chip_fs, chip_fr, at_chip(other)
        )

    def out_copy(i, other):
        to, slot = i * chips + other, i * chips + chip
        return remote(to_chips.at[to], from_chips.at[slot], out_s, out_r.at[i], at_chip(other))

    def out_copies(count, recv):
        taken = pl.ds(0, count)
        return remote(to_chips.at[taken], from_chips.at[taken], out_s, recv, at_core())

    def send_out(i, other):
        @pl.when(jnp.logical_not(last))
        def _():
            out_copy(i, other).start()

    def combine(i, send):
        core_copy(i).wait_recv()
        waiting = None
        for m in hops + [0]:
            other = partner(m) if m else chip
            head = i * chips + other
            factor = jnp.exp(own_fin[other, pl.ds(i, 1), :])
            total = (terms[kind, head] + factor * from_core[head]).astype(BF16)
            if m:
                to_chips[head] = total
            else:
                from_chips[head] = total
            if send and waiting is not None:
                send_out(i, waiting)
            waiting = other

    def plane_fin_copy(plane, side):
        to = (plane, chip * 2 + side)
        return remote(plane_fin.at[z], plane_fin.at[z], plane_fs, plane_fr, to)

    share_copy = remote(chip_fin, chip_fin, share_s, share_r, at_core())

    def planes_step(_):
        taken = chip_fin.at[pl.ds(0, chips - 1)]
        remote(taken, taken, chip_fs, chip_fr, at_core()).wait_recv()
        total = chip_fin[0]
        for other in range(1, chips):
            total = total + chip_fin[other]
        plane_fin[z] = total
        share_copy.start()
        for step in range(1, planes):
            for side in range(2):
                plane_fin_copy(lax.rem(z + step, planes), side).start()

    def plane_copy(i, other):
        return remote(
            plane_sum.at[i], from_planes.at[z, i], plane_s, plane_r.at[i], at_plane(other)
        )

    def factor_of(fins, at, i):
        return jnp.exp(fins[at, pl.ds(i, 1), :])

    def sum_step(i):
        fewer = (depth == planes - 1) & (spot < chips - 1)
        for few, count in ((fewer, chips - 2), (jnp.logical_not(fewer), chips - 1)):
            @pl.when(few)
            def _():
                out_copies(count, out_r.at[i]).wait_recv()

        @pl.when(depth < planes - 1)
        def _():
            total = from_chips[i * chips + place(0)].astype(F32)
            for j in range(1, chips):
                at = place(j)
                total = total * factor_of(chip_fin, at, i) + from_chips[i * chips + at].astype(F32)
            plane_sum[i] = total.astype(BF16)

            @pl.loop(0, planes - 1 - depth)
            def _(j):
                plane_copy(i, level(planes - 1 - j)).start()

    def back_copy(i, other):
        to, slot = i * chips + other, i * chips + chip
        return remote(to_back.at[to], raw.at[slot], back_s, back_r.at[i], at_chip(other))

    def back_copies(count, recv):
        taken = pl.ds(0, count)
        return remote(to_back.at[taken], raw.at[taken], back_s, recv, at_core())

    def carry_step(i):
        head = i * chips + chip
        if i == 0:
            taken = plane_fin.at[pl.ds(0, planes - 1)]
            remote(taken, taken, plane_fs, plane_fr, at_core()).wait_recv()
        for count in range(1, planes):
            @pl.when(depth == count)
            def _():
                taken = from_planes.at[pl.ds(0, count), i]
                remote(taken, taken, plane_s, plane_r.at[i], at_core()).wait_recv()

        def add_plane(j, state):
            at = level(j)
            return state * factor_of(plane_fin, at, i) + from_planes[at, i].astype(F32)

        state = lax.fori_loop(0, depth, add_plane, jnp.zeros((SIZE, SIZE), F32))
        for j in range(chips):
            at = place(j)
            to_back[i * chips + at] = state.astype(BF16)
            if j < chips - 1:
                state = state * factor_of(chip_fin, at, i) + from_chips[i * chips + at].astype(F32)
        for m in hops:
            other = partner(m)

            @pl.when((depth > 0) | (other != place(0)))
            def _():
                back_copy(i, other).start()
        raw[head] = to_back[head]

    def last_copy(i):
        taken = pl.ds(i * chips, chips)
        return remote(raw.at[taken], states.at[taken], last_s, last_r.at[i], at_core())

    def apply(which, head, state):
        taken = columns(head)
        scale = scales[which, head]
        straight = dot(held[which, :, taken], state)
        out_ref[which, :, taken] = (local[which, head] + scale * straight).astype(BF16)
        turned = over_columns(held[2 + which, :, taken], state)
        out_ref[2 + which, :, taken] = (local[2 + which, head] + scale * turned).astype(BF16)

    def pass_step(i):
        @pl.when(jnp.logical_not(first))
        def _():
            back_copies(chips - 1, back_r.at[i]).wait_recv()
        last_copy(i).start()
        for o in range(chips):
            head = i * chips + o
            factor = jnp.exp(core_fin[o, pl.ds(i, 1), :])
            apply(kind, head, (factor * raw[head].astype(F32) + from_core[head]).astype(BF16))

    def other_step(i):
        last_copy(i).wait_recv()
        for o in range(chips):
            head = i * chips + o
            apply(core, head, states[head])

    @pl.when(first)
    def _():
        @pl.loop(0, heads)
        def _(head):
            raw[head] = jnp.zeros((SIZE, SIZE), BF16)

    parts = heads // 2

    def inside_step(part):
        for j in range(2):
            inside(part * 2 + j)

    def lead_turn(_):
        pl.semaphore_signal(go_s, inc=1, device_id=at_core(), device_id_type=MESH)

    def tail_turn(_):
        pl.semaphore_wait(go_s, 1)
        for i in range(own):
            for m in hops:
                send_out(i, partner(m))

    steps = {
        "planes": planes_step, "sum": sum_step, "carry": carry_step, "pass": pass_step,
        "other": other_step, "inside": inside_step,
    }

    @pl.when(lead)
    def _():
        half = own // 2
        pl.loop(0, half)(terms_step)
        pl.semaphore_wait(barrier, 2 * (chips + planes) - 3)
        fin_copy.start()
        for i in range(half):
            core_copy(i).start()
        fin_copy.wait_recv()
        chip_total[...] = own_fin[...] + core_fin[...]
        chip_fin[chip] = chip_total[chip]
        terms_step(half)
        core_copy(half).start()
        for m in hops:
            chip_fin_copy(partner(m)).start()
        combine(0, True)
        for i in range(half + 1, own):
            terms_step(i)
            core_copy(i).start()
            combine(i - half, True)
        for i in range(own - half, own):
            combine(i, True)
        for step, i in lead_plan(own, parts):
            {**steps, "turn": lead_turn}[step](i)
        taken = chip_fin.at[pl.ds(0, chips - 1)]
        remote(taken, taken, chip_fs, chip_fr, at_core()).wait_send()
        share_copy.wait_send()
        for _ in range(2):
            taken = plane_fin.at[pl.ds(0, planes - 1)]
            remote(taken, taken, plane_fs, plane_fr, at_core()).wait_send()

    @pl.when(jnp.logical_not(lead))
    def _():
        pl.semaphore_wait(barrier, 1)
        fin_copy.start()

        @pl.loop(0, own)
        def _(i):
            terms_step(i)
            core_copy(i).start()

        fin_copy.wait_recv()
        tail = {
            "turn": tail_turn, "combine": lambda i: combine(i, False),
            "share": lambda _: share_copy.wait_recv(),
        }
        for step, i in tail_plan(own, parts):
            {**steps, **tail}[step](i)

    fin_copy.wait_send()
    core_copies(0, heads, core_r.at[0]).wait_send()

    @pl.when(jnp.logical_not(last))
    def _():
        out_copies(own * (chips - 1), out_r.at[0]).wait_send()
    fewer = (depth == 0) & (spot > 0)
    for few, count in ((fewer, chips - 2), (jnp.logical_not(fewer), chips - 1)):
        @pl.when(few)
        def _():
            back_copies(own * count, back_r.at[0]).wait_send()
    remote(raw, states, last_s, last_r.at[0], at_core()).wait_send()
    for count in range(1, planes):
        @pl.when(planes - 1 - depth == count)
        def _():
            taken = from_planes.at[pl.ds(0, count)]
            remote(taken, taken, plane_s, plane_r.at[0], at_core()).wait_send()


def computed(planes, devices, arrays):
    decay = pltpu.with_memory_space_constraint(arrays[-1].T, pltpu.HBM)
    arrays = [pltpu.with_memory_space_constraint(item, pltpu.HBM) for item in arrays[:-1]] + [decay]
    heads, rows = decay.shape
    chips = devices // 2
    own = heads // chips
    square = (SIZE, SIZE)
    wide = arrays[0].shape
    dma = pltpu.SemaphoreType.DMA
    return pl.pallas_call(
        functools.partial(main_kernel, planes, devices),
        out_shape=jax.ShapeDtypeStruct((4,) + wide, BF16),
        in_specs=[pl.BlockSpec(memory_space=pltpu.HBM)] * 5,
        out_specs=pl.BlockSpec(memory_space=pltpu.VMEM),
        scratch_shapes=[
            pltpu.VMEM((4,) + wide, BF16),
            pltpu.VMEM((heads, rows), BF16),
            pltpu.VMEM((heads, rows), F32),
            pltpu.VMEM((heads, rows), F32),
            pltpu.VMEM((heads, rows), F32),
            pltpu.VMEM((2, heads, rows, SIZE), F32),
            pltpu.VMEM((4, heads) + square, F32),
            pltpu.VMEM((2, heads) + square, F32),
            pltpu.VMEM((heads,) + square, F32),
            pltpu.VMEM((heads,) + square, BF16),
            pltpu.VMEM((heads,) + square, BF16),
            pltpu.VMEM((own,) + square, BF16),
            pltpu.VMEM((planes, own) + square, BF16),
            pltpu.VMEM((heads,) + square, BF16),
            pltpu.VMEM((heads,) + square, BF16),
            pltpu.VMEM((heads,) + square, BF16),
            pltpu.VMEM((chips, own, SIZE), F32),
            pltpu.VMEM((chips, own, SIZE), F32),
            pltpu.VMEM((chips, own, SIZE), F32),
            pltpu.VMEM((chips, own, SIZE), F32),
            pltpu.VMEM((planes, own, SIZE), F32),
            dma((own,)), dma, pltpu.SemaphoreType.REGULAR, dma, dma, dma, dma, dma, dma, dma, dma,
            dma, dma((own,)), dma, dma((own,)), dma, dma((own,)),
            dma, dma((own,)), dma, dma((own,)),
        ],
        compiler_params=pltpu.CompilerParams(
            collective_id=0, has_side_effects=True, vmem_limit_bytes=48 * 2**20
        ),
    )(*arrays)


def store_kernel(held, o_out, dq_out, dk_out, dv_out, store_s):
    copies = [
        pltpu.make_async_copy(held.at[j], dst, store_s.at[j])
        for j, dst in enumerate((o_out, dv_out, dq_out, dk_out))
    ]
    for copy in copies:
        copy.start()
    for copy in copies:
        copy.wait()


def stored(results):
    return pl.pallas_call(
        store_kernel,
        out_shape=[jax.ShapeDtypeStruct(results.shape[1:], BF16)] * 4,
        in_specs=[pl.BlockSpec(memory_space=pltpu.VMEM)],
        out_specs=[pl.BlockSpec(memory_space=pltpu.HBM)] * 4,
        scratch_shapes=[pltpu.SemaphoreType.DMA((4,))],
        compiler_params=pltpu.CompilerParams(vmem_limit_bytes=2 * 2**20),
    )(results)


def solution(mesh):
    planes, devices = mesh.shape["chain"], mesh.shape["inner"]

    def shards(*arrays):
        return tuple(stored(computed(planes, devices, arrays)))

    spec = P(("chain", "inner"), None)
    return jax.shard_map(
        shards, mesh=mesh, in_specs=(spec,) * 5, out_specs=(spec,) * 4, check_vma=False
    )
```

```python
import functools

import jax
import jax.numpy as jnp
from jax import lax
from jax.experimental import pallas as pl
from jax.experimental.pallas import tpu as pltpu
from jax.sharding import PartitionSpec as P

SIZE = 128
F32 = jnp.float32
BF16 = jnp.bfloat16
MESH = pl.DeviceIdType.MESH
LAG = 1


def lower_triangle(rows):
    row = lax.broadcasted_iota(jnp.int32, (rows, rows), 0)
    column = lax.broadcasted_iota(jnp.int32, (rows, rows), 1)
    return row >= column


def over_rows(left, right):
    return lax.dot_general(left, right, (((0,), (0,)), ((), ())), preferred_element_type=F32)


def over_columns(left, right):
    return lax.dot_general(left, right, (((1,), (1,)), ((), ())), preferred_element_type=F32)


def dot(left, right):
    return jnp.dot(left, right, preferred_element_type=F32)


def plan(ready, rounds, parts, now):
    ready = sorted(ready)
    order, part = [], 0
    while ready:
        if ready[0][0] > now + 0.1 and part < parts:
            order.append(("inside", part))
            now += 10.0 / parts
            part += 1
            continue
        at, length, step, i = ready.pop(0)
        if step in ("pass", "other"):
            while part < min(parts, -(-parts * (i + 1) // rounds)):
                order.append(("inside", part))
                now += 10.0 / parts
                part += 1
        order.append((step, i))
        now = max(now, at) + length
    return order


def lead_plan(rounds, parts):
    ready = [(7.5, 0.1, "planes", 0)]
    for i in range(rounds):
        ready.append((7.8 + 0.7 * i, 0.15, "sum", i))
        ready.append((13.2 + 0.7 * i, 0.35, "carry", i))
        ready.append((19.0 + 0.7 * i, 0.55, "pass", i))
        ready.append((25.7 + 0.7 * i, 0.35, "other", i))
    turn = min(2, rounds - 1)
    ready.append((7.81 + 0.7 * turn, 0.01, "turn", 0))
    return plan(ready, rounds, parts, 6.7)


def tail_plan(rounds, parts):
    ready = [(7.9, 0.1, "turn", 0), (13.3, 0.05, "share", 0)]
    for i in range(rounds):
        ready.append((5.1 + 0.3 * i, 0.3, "combine", i))
        ready.append((13.4 + 0.7 * i, 0.15, "sum", i))
        ready.append((17.5 + 0.7 * i, 0.35, "carry", i))
        ready.append((24.6 + 0.7 * i, 0.55, "pass", i))
        ready.append((20.1 + 0.7 * i, 0.35, "other", i))
    return plan(ready, rounds, parts, 4.5)


def late_kind(plane, planes):
    return jnp.where(plane * 2 < planes, 1, 0)


def apply_state(which, head, place, state, held, scales, local, out_ref):
    taken = pl.ds(pl.multiple_of(head * SIZE, SIZE), SIZE)
    scale = scales[which, head]
    straight = dot(held[which, :, taken], state)
    out_ref(0, place, (local[which, head] + scale * straight).astype(BF16))
    turned = over_columns(held[2 + which, :, taken], state)
    out_ref(2, place, (local[2 + which, head] + scale * turned).astype(BF16))


def main_kernel(
    planes, devices, q_any, k_any, v_any, g_any, d_any, out_ref, held, scales, local, states,
    d_ref, decay_rows, forward_rows, backward_rows, terms, from_core,
    to_chips, from_chips, plane_sum, from_planes, to_back, raw,
    own_fin, core_fin, chip_total, chip_fin, plane_fin,
    load_s, decay_s, go_s, fin_s, fin_r, chip_fs, chip_fr, plane_fs, plane_fr, share_s, share_r,
    core_s, core_r, out_s, out_r, plane_s, plane_r, back_s, back_r, late_r, last_s, last_r,
):
    heads, rows = d_any.shape
    chips = devices // 2
    own = heads // chips
    z = lax.axis_index("chain")
    me = lax.axis_index("inner")
    chip, core = me // 2, lax.rem(me, 2)
    kind = 1 - core
    ahead = core == 1

    def place(j):
        return jnp.where(ahead, j, chips - 1 - j)

    def level(j):
        return jnp.where(ahead, j, planes - 1 - j)

    depth, spot = level(z), place(chip)

    def lead_core(plane):
        return late_kind(plane, planes)

    lead = core == lead_core(z)
    first = (depth == 0) & (spot == 0)
    last = (depth == planes - 1) & (spot == chips - 1)

    def partner(m):
        if chips & (chips - 1):
            return lax.rem(chip + m, chips)
        bits = [(1 << b, (m >> b) & 1) for b in range(chips.bit_length() - 1)]
        return sum(lax.rem(chip // size + bit, 2) * size for size, bit in bits)

    hops = sorted(range(1, chips), key=lambda m: -bin(m).count("1"))

    def at_core():
        return (z, chip * 2 + 1 - core)

    def at_chip(other):
        return (z, other * 2 + core)

    def at_plane(other):
        return (other, me)

    def remote(src, dst, send, recv, to):
        return pltpu.make_async_remote_copy(
            src_ref=src, dst_ref=dst, send_sem=send, recv_sem=recv, device_id=to, device_id_type=MESH
        )

    def columns(head):
        return pl.ds(pl.multiple_of(head * SIZE, SIZE), SIZE)

    def round_columns(i):
        return pl.ds(pl.multiple_of(i * (chips * SIZE), SIZE), chips * SIZE)

    decay_load = pltpu.make_async_copy(d_any, d_ref, decay_s)
    decay_load.start()

    @pl.loop(0, own)
    def _(i):
        taken = round_columns(i)
        for j, src in enumerate((q_any, k_any, g_any, v_any)):
            pltpu.make_async_copy(src.at[:, taken], held.at[j, :, taken], load_s.at[i]).start()

    barrier = pltpu.get_barrier_semaphore()

    def greet(to):
        pl.semaphore_signal(barrier, inc=1, device_id=to, device_id_type=MESH)

    for step in range(1, planes):
        plane = lax.rem(z + step, planes)
        greet((plane, chip * 2 + lead_core(plane)))
    for m in hops:
        greet((z, partner(m) * 2 + lead_core(z)))
    greet(at_core())

    lower = lower_triangle(rows)
    row = lax.broadcasted_iota(jnp.int32, (rows, rows), 0)
    column = lax.broadcasted_iota(jnp.int32, (rows, rows), 1)
    upto = (row <= column).astype(F32).astype(BF16)
    after = (row > column).astype(F32).astype(BF16)
    ones = jnp.ones((rows, SIZE), BF16)
    row = lax.broadcasted_iota(jnp.int32, (heads, heads), 0)
    column = lax.broadcasted_iota(jnp.int32, (heads, heads), 1)
    owners = (column == (row % own) * chips + row // own).astype(F32).astype(BF16)

    decay_load.wait()
    decay = d_ref[...]
    decay_rows[...] = decay.astype(F32)
    by_owner = dot(dot(owners, decay).astype(BF16), ones)
    for o in range(chips):
        own_fin[o] = by_owner[o * own : (o + 1) * own]
    fin = dot(decay, ones)
    cumul = dot(decay, upto)
    forward_rows[...] = jnp.exp(cumul)
    backward_rows[...] = jnp.exp(fin - cumul)

    fin_copy = remote(own_fin, core_fin, fin_s, fin_r, at_core())

    def core_copies(begin, count, recv):
        taken = pl.ds(begin, count)
        return remote(terms.at[core, taken], from_core.at[taken], core_s, recv, at_core())

    def core_copy(i):
        return core_copies(i * chips, chips, core_r.at[i])

    def make_terms(head):
        taken = columns(head)
        keys = held[1, :, taken].T.astype(F32) * backward_rows[pl.ds(head, 1), :]
        terms[0, head] = dot(keys.astype(BF16), held[3, :, taken])
        queries = held[0, :, taken].T.astype(F32) * forward_rows[pl.ds(head, 1), :]
        terms[1, head] = dot(queries.astype(BF16), held[2, :, taken])

    def terms_step(i):
        part = held.at[:, :, round_columns(i)]
        pltpu.make_async_copy(part, part, load_s.at[i]).wait()
        for o in range(chips):
            make_terms(i * chips + o)

    def inside(head):
        taken = columns(head)
        query, key, grad, value = (held[j, :, taken] for j in range(4))
        picked = jnp.where(lower, decay_rows[pl.ds(head, 1), :], 0.0).astype(BF16)
        spans = dot(picked, jnp.concatenate([after, ones], axis=1))
        weights = jnp.where(lower, jnp.exp(spans[:, :rows]), 0.0)
        sums = spans[:, rows:]
        scales[0, head] = jnp.exp(sums)
        scales[1, head] = jnp.exp(own_fin[lax.rem(head, chips), pl.ds(head // chips, 1), :] - sums)
        probs = (over_columns(query, key) * weights).astype(BF16)
        grows = (over_columns(grad, value) * weights).astype(BF16)
        local[0, head] = dot(probs, value)
        local[1, head] = over_rows(probs, grad)
        local[2, head] = dot(grows, key)
        local[3, head] = over_rows(grows, query)

    def chip_fin_copy(other):
        return remote(
            chip_total.at[other], chip_fin.at[chip], chip_fs, chip_fr, at_chip(other)
        )

    def out_copy(i, other):
        to, slot = i * chips + other, i * chips + chip
        return remote(to_chips.at[to], from_chips.at[slot], out_s, out_r.at[i], at_chip(other))

    def out_copies(count, recv):
        taken = pl.ds(0, count)
        return remote(to_chips.at[taken], from_chips.at[taken], out_s, recv, at_core())

    def send_out(i, other):
        @pl.when(jnp.logical_not(last))
        def _():
            out_copy(i, other).start()

    def combine(i, send):
        core_copy(i).wait_recv()
        waiting = None
        for m in hops + [0]:
            other = partner(m) if m else chip
            head = i * chips + other
            factor = jnp.exp(own_fin[other, pl.ds(i, 1), :])
            total = (terms[kind, head] + factor * from_core[head]).astype(BF16)
            if m:
                to_chips[head] = total
            else:
                from_chips[head] = total
            if send and waiting is not None:
                send_out(i, waiting)
            waiting = other

    def plane_fin_copy(plane, side):
        to = (plane, chip * 2 + side)
        return remote(plane_fin.at[z], plane_fin.at[z], plane_fs, plane_fr, to)

    share_copy = remote(chip_fin, chip_fin, share_s, share_r, at_core())

    def planes_step(_):
        taken = chip_fin.at[pl.ds(0, chips - 1)]
        remote(taken, taken, chip_fs, chip_fr, at_core()).wait_recv()
        total = chip_fin[0]
        for other in range(1, chips):
            total = total + chip_fin[other]
        plane_fin[z] = total
        share_copy.start()
        for step in range(1, planes):
            for side in range(2):
                plane_fin_copy(lax.rem(z + step, planes), side).start()

    def plane_copy(i, other):
        return remote(
            plane_sum.at[i], from_planes.at[z, i], plane_s, plane_r.at[i], at_plane(other)
        )

    def factor_of(fins, at, i):
        return jnp.exp(fins[at, pl.ds(i, 1), :])

    def sum_step(i):
        fewer = (depth == planes - 1) & (spot < chips - 1)
        for few, count in ((fewer, chips - 2), (jnp.logical_not(fewer), chips - 1)):
            @pl.when(few)
            def _():
                out_copies(count, out_r.at[i]).wait_recv()

        @pl.when(depth < planes - 1)
        def _():
            total = from_chips[i * chips + place(0)].astype(F32)
            for j in range(1, chips):
                at = place(j)
                total = total * factor_of(chip_fin, at, i) + from_chips[i * chips + at].astype(F32)
            plane_sum[i] = total.astype(BF16)

            @pl.loop(0, planes - 1 - depth)
            def _(j):
                plane_copy(i, level(planes - 1 - j)).start()

    def back_copy(i, other):
        to, slot = i * chips + other, i * chips + chip
        recv = back_r.at[i] if i < own - 1 else late_r.at[chip]
        return remote(to_back.at[to], raw.at[slot], back_s, recv, at_chip(other))

    def back_copies(count, recv):
        taken = pl.ds(0, count)
        return remote(to_back.at[taken], raw.at[taken], back_s, recv, at_core())

    def send_back(i, to_first):
        for m in hops:
            other = partner(m)
            wanted = (depth > 0) | (other != place(0))
            if to_first is not None:
                wanted = wanted & ((other == 0) if to_first else (other != 0))

            @pl.when(wanted)
            def _():
                back_copy(i, other).start()

    def carry_step(i, lag=0):
        head = i * chips + chip
        if i == 0:
            taken = plane_fin.at[pl.ds(0, planes - 1)]
            remote(taken, taken, plane_fs, plane_fr, at_core()).wait_recv()
        for count in range(1, planes):
            @pl.when(depth == count)
            def _():
                taken = from_planes.at[pl.ds(0, count), i]
                remote(taken, taken, plane_s, plane_r.at[i], at_core()).wait_recv()

        def add_plane(j, state):
            at = level(j)
            return state * factor_of(plane_fin, at, i) + from_planes[at, i].astype(F32)

        state = lax.fori_loop(0, depth, add_plane, jnp.zeros((SIZE, SIZE), F32))
        for j in range(chips):
            at = place(j)
            to_back[i * chips + at] = state.astype(BF16)
            if j < chips - 1:
                state = state * factor_of(chip_fin, at, i) + from_chips[i * chips + at].astype(F32)
        if lag == 0:
            send_back(i, None)
        else:
            send_back(i, True)
            if i >= lag:
                send_back(i - lag, False)
            if i == own - 1:
                for late in range(max(own - lag, 0), own):
                    send_back(late, False)
        raw[head] = to_back[head]

    def last_part(i, other):
        head = i * chips + other
        return remote(raw.at[head], states.at[head], last_s, last_r.at[i], at_core())

    def last_copy(i):
        taken = pl.ds(i * chips, chips)
        return remote(raw.at[taken], states.at[taken], last_s, last_r.at[i], at_core())

    def apply(which, head, state):
        def put(j, taken, value):
            out_ref[j + which, :, taken] = value

        apply_state(which, head, columns(head), state, held, scales, local, put)

    def pass_step(i, late):
        if i < own - 1:
            @pl.when(jnp.logical_not(first))
            def _():
                back_copies(chips - 1, back_r.at[i]).wait_recv()
            last_copy(i).start()
        else:
            last_part(i, chip).start()
            for m in hops:
                other = partner(m)

                @pl.when(jnp.logical_not(first))
                def _():
                    back_copies(1, late_r.at[other]).wait_recv()
                last_part(i, other).start()
        for o in range(chips):
            head = i * chips + o
            factor = jnp.exp(core_fin[o, pl.ds(i, 1), :])
            state = (factor * raw[head].astype(F32) + from_core[head]).astype(BF16)
            if late and i == own - 1:
                states[head] = state
            else:
                apply(kind, head, state)

    def other_step(i, late):
        last_copy(i).wait_recv()
        if late and i == own - 1:
            return
        for o in range(chips):
            head = i * chips + o
            apply(core, head, states[head])

    @pl.when(first)
    def _():
        @pl.loop(0, heads)
        def _(head):
            raw[head] = jnp.zeros((SIZE, SIZE), BF16)

    parts = heads // 2

    def inside_step(part):
        for j in range(2):
            inside(part * 2 + j)

    def lead_turn(_):
        pl.semaphore_signal(go_s, inc=1, device_id=at_core(), device_id_type=MESH)

    def tail_turn(_):
        pl.semaphore_wait(go_s, 1)
        for i in range(own):
            for m in hops:
                send_out(i, partner(m))

    steps = {
        "planes": planes_step, "sum": sum_step, "carry": carry_step, "inside": inside_step,
    }

    @pl.when(lead)
    def _():
        half = own // 2
        pl.loop(0, half)(terms_step)
        pl.semaphore_wait(barrier, 2 * (chips + planes) - 3)
        fin_copy.start()
        for i in range(half):
            core_copy(i).start()
        fin_copy.wait_recv()
        chip_total[...] = own_fin[...] + core_fin[...]
        chip_fin[chip] = chip_total[chip]
        terms_step(half)
        core_copy(half).start()
        for m in hops:
            chip_fin_copy(partner(m)).start()
        combine(0, True)
        for i in range(half + 1, own):
            terms_step(i)
            core_copy(i).start()
            combine(i - half, True)
        for i in range(own - half, own):
            combine(i, True)
        front = {
            "turn": lead_turn, "pass": lambda i: pass_step(i, False),
            "other": lambda i: other_step(i, True),
        }
        for step, i in lead_plan(own, parts):
            {**steps, **front}[step](i)
        taken = chip_fin.at[pl.ds(0, chips - 1)]
        remote(taken, taken, chip_fs, chip_fr, at_core()).wait_send()
        share_copy.wait_send()
        for _ in range(2):
            taken = plane_fin.at[pl.ds(0, planes - 1)]
            remote(taken, taken, plane_fs, plane_fr, at_core()).wait_send()

    @pl.when(jnp.logical_not(lead))
    def _():
        pl.semaphore_wait(barrier, 1)
        fin_copy.start()

        @pl.loop(0, own)
        def _(i):
            terms_step(i)
            core_copy(i).start()

        fin_copy.wait_recv()
        tail = {
            "turn": tail_turn, "combine": lambda i: combine(i, False),
            "share": lambda _: share_copy.wait_recv(), "carry": lambda i: carry_step(i, LAG),
            "pass": lambda i: pass_step(i, True), "other": lambda i: other_step(i, False),
        }
        for step, i in tail_plan(own, parts):
            {**steps, **tail}[step](i)

    fin_copy.wait_send()
    core_copies(0, heads, core_r.at[0]).wait_send()

    @pl.when(jnp.logical_not(last))
    def _():
        out_copies(own * (chips - 1), out_r.at[0]).wait_send()
    fewer = (depth == 0) & (spot > 0)
    for few, count in ((fewer, chips - 2), (jnp.logical_not(fewer), chips - 1)):
        @pl.when(few)
        def _():
            back_copies(own * count, back_r.at[0]).wait_send()
    remote(raw, states, last_s, last_r.at[0], at_core()).wait_send()
    for count in range(1, planes):
        @pl.when(planes - 1 - depth == count)
        def _():
            taken = from_planes.at[pl.ds(0, count)]
            remote(taken, taken, plane_s, plane_r.at[0], at_core()).wait_send()


def computed(planes, devices, arrays):
    decay = pltpu.with_memory_space_constraint(arrays[-1].T, pltpu.HBM)
    arrays = [pltpu.with_memory_space_constraint(item, pltpu.HBM) for item in arrays[:-1]] + [decay]
    heads, rows = decay.shape
    chips = devices // 2
    own = heads // chips
    square = (SIZE, SIZE)
    wide = arrays[0].shape
    dma = pltpu.SemaphoreType.DMA
    return pl.pallas_call(
        functools.partial(main_kernel, planes, devices),
        out_shape=[
            jax.ShapeDtypeStruct((4,) + wide, BF16),
            jax.ShapeDtypeStruct((4,) + wide, BF16),
            jax.ShapeDtypeStruct((2, heads, rows, SIZE), F32),
            jax.ShapeDtypeStruct((4, heads) + square, F32),
            jax.ShapeDtypeStruct((heads,) + square, BF16),
        ],
        in_specs=[pl.BlockSpec(memory_space=pltpu.HBM)] * 5,
        out_specs=[pl.BlockSpec(memory_space=pltpu.VMEM)] * 5,
        scratch_shapes=[
            pltpu.VMEM((heads, rows), BF16),
            pltpu.VMEM((heads, rows), F32),
            pltpu.VMEM((heads, rows), F32),
            pltpu.VMEM((heads, rows), F32),
            pltpu.VMEM((2, heads) + square, F32),
            pltpu.VMEM((heads,) + square, F32),
            pltpu.VMEM((heads,) + square, BF16),
            pltpu.VMEM((heads,) + square, BF16),
            pltpu.VMEM((own,) + square, BF16),
            pltpu.VMEM((planes, own) + square, BF16),
            pltpu.VMEM((heads,) + square, BF16),
            pltpu.VMEM((heads,) + square, BF16),
            pltpu.VMEM((chips, own, SIZE), F32),
            pltpu.VMEM((chips, own, SIZE), F32),
            pltpu.VMEM((chips, own, SIZE), F32),
            pltpu.VMEM((chips, own, SIZE), F32),
            pltpu.VMEM((planes, own, SIZE), F32),
            dma((own,)), dma, pltpu.SemaphoreType.REGULAR, dma, dma, dma, dma, dma, dma, dma, dma,
            dma, dma((own,)), dma, dma((own,)), dma, dma((own,)),
            dma, dma((own,)), dma((chips,)), dma, dma((own,)),
        ],
        compiler_params=pltpu.CompilerParams(
            collective_id=0, has_side_effects=True, vmem_limit_bytes=20 * 2**20
        ),
    )(*arrays)


def store_kernel(
    planes, chips, done, held, scales, local, states, o_out, dq_out, dk_out, dv_out, fresh, store_s, late_s
):
    heads = states.shape[0]
    width = chips * SIZE
    split = heads * SIZE - width
    which = late_kind(lax.axis_index("chain"), planes)
    outs = (o_out, dv_out, dq_out, dk_out)
    early, late = pl.ds(0, split), pl.ds(split, width)
    copies = [
        pltpu.make_async_copy(done.at[j, :, early], dst.at[:, early], store_s.at[j])
        for j, dst in enumerate(outs)
    ]
    for copy in copies:
        copy.start()

    def late_copies(kind):
        pairs = []
        for j in range(2):
            pairs.append((fresh.at[j], outs[2 * j + kind]))
            pairs.append((done.at[2 * j + 1 - kind, :, late], outs[2 * j + 1 - kind]))
        return [
            pltpu.make_async_copy(src, dst.at[:, late], late_s.at[j])
            for j, (src, dst) in enumerate(pairs)
        ]

    def put(j, taken, value):
        fresh[j // 2, :, taken] = value

    for o in range(chips):
        head = heads - chips + o
        apply_state(which, head, pl.ds(o * SIZE, SIZE), states[head], held, scales, local, put)
    for kind in range(2):
        @pl.when(which == kind)
        def _():
            for copy in late_copies(kind):
                copy.start()
            for copy in late_copies(kind):
                copy.wait()
    for copy in copies:
        copy.wait()


def stored(planes, chips, results):
    rows, features = results[0].shape[1:]
    return pl.pallas_call(
        functools.partial(store_kernel, planes, chips),
        out_shape=[jax.ShapeDtypeStruct((rows, features), BF16)] * 4,
        in_specs=[pl.BlockSpec(memory_space=pltpu.VMEM)] * 5,
        out_specs=[pl.BlockSpec(memory_space=pltpu.HBM)] * 4,
        scratch_shapes=[
            pltpu.VMEM((2, rows, chips * SIZE), BF16),
            pltpu.SemaphoreType.DMA((4,)),
            pltpu.SemaphoreType.DMA((4,)),
        ],
        compiler_params=pltpu.CompilerParams(vmem_limit_bytes=4 * 2**20),
    )(*results)


def solution(mesh):
    planes, devices = mesh.shape["chain"], mesh.shape["inner"]

    def shards(*arrays):
        return tuple(stored(planes, devices // 2, computed(planes, devices, arrays)))

    spec = P(("chain", "inner"), None)
    return jax.shard_map(
        shards, mesh=mesh, in_specs=(spec,) * 5, out_specs=(spec,) * 4, check_vma=False
    )
```

```python
import functools

import jax
import jax.numpy as jnp
from jax import lax
from jax.experimental import pallas as pl
from jax.experimental.pallas import tpu as pltpu
from jax.sharding import PartitionSpec as P

SIZE = 128
F32 = jnp.float32
BF16 = jnp.bfloat16
MESH = pl.DeviceIdType.MESH
LAG = 1


def lower_triangle(rows):
    row = lax.broadcasted_iota(jnp.int32, (rows, rows), 0)
    column = lax.broadcasted_iota(jnp.int32, (rows, rows), 1)
    return row >= column


def over_rows(left, right):
    return lax.dot_general(left, right, (((0,), (0,)), ((), ())), preferred_element_type=F32)


def over_columns(left, right):
    return lax.dot_general(left, right, (((1,), (1,)), ((), ())), preferred_element_type=F32)


def dot(left, right):
    return jnp.dot(left, right, preferred_element_type=F32)


def plan(ready, rounds, parts, now):
    ready = sorted(ready)
    order, part = [], 0
    while ready:
        if ready[0][0] > now + 0.1 and part < parts:
            order.append(("inside", part))
            now += 10.0 / parts
            part += 1
            continue
        at, length, step, i = ready.pop(0)
        if step in ("pass", "other"):
            while part < min(parts, -(-parts * (i + 1) // rounds)):
                order.append(("inside", part))
                now += 10.0 / parts
                part += 1
        order.append((step, i))
        now = max(now, at) + length
    return order


def lead_plan(rounds, parts):
    ready = [(7.5, 0.1, "planes", 0)]
    for i in range(rounds):
        ready.append((7.8 + 0.7 * i, 0.15, "sum", i))
        ready.append((13.2 + 0.7 * i, 0.35, "carry", i))
        ready.append((19.0 + 0.7 * i, 0.55, "pass", i))
        ready.append((25.7 + 0.7 * i, 0.35, "other", i))
    turn = min(2, rounds - 1)
    ready.append((7.81 + 0.7 * turn, 0.01, "turn", 0))
    return plan(ready, rounds, parts, 6.7)


def tail_plan(rounds, parts):
    ready = [(7.9, 0.1, "turn", 0), (13.3, 0.05, "share", 0)]
    for i in range(rounds):
        ready.append((5.1 + 0.3 * i, 0.3, "combine", i))
        ready.append((13.4 + 0.7 * i, 0.15, "sum", i))
        ready.append((17.5 + 0.7 * i, 0.35, "carry", i))
        ready.append((24.6 + 0.7 * i, 0.55, "pass", i))
        ready.append((20.1 + 0.7 * i, 0.35, "other", i))
    return plan(ready, rounds, parts, 4.5)


def late_kind(plane, planes):
    return jnp.where(plane * 2 < planes, 1, 0)


def apply_state(which, head, place, state, held, scales, local, out_ref):
    taken = pl.ds(pl.multiple_of(head * SIZE, SIZE), SIZE)
    scale = scales[which, head]
    straight = dot(held[which, :, taken], state)
    out_ref(0, place, (local[which, head] + scale * straight).astype(BF16))
    turned = over_columns(held[2 + which, :, taken], state)
    out_ref(2, place, (local[2 + which, head] + scale * turned).astype(BF16))


def main_kernel(
    planes, devices, q_any, k_any, v_any, g_any, d_any, out_ref, held, scales, local, states,
    d_ref, decay_rows, forward_rows, backward_rows, terms, from_core,
    to_chips, from_chips, plane_sum, from_planes, to_back, raw,
    own_fin, core_fin, chip_total, chip_fin, plane_fin,
    load_s, decay_s, go_s, fin_s, fin_r, chip_fs, chip_fr, plane_fs, plane_fr, share_s, share_r,
    core_s, core_r, out_s, out_r, plane_s, plane_r, back_s, back_r, late_r, last_s,
):
    heads, rows = d_any.shape
    chips = devices // 2
    own = heads // chips
    z = lax.axis_index("chain")
    me = lax.axis_index("inner")
    chip, core = me // 2, lax.rem(me, 2)
    kind = 1 - core
    ahead = core == 1

    def place(j):
        return jnp.where(ahead, j, chips - 1 - j)

    def level(j):
        return jnp.where(ahead, j, planes - 1 - j)

    depth, spot = level(z), place(chip)

    def lead_core(plane):
        return late_kind(plane, planes)

    lead = core == lead_core(z)
    first = (depth == 0) & (spot == 0)
    last = (depth == planes - 1) & (spot == chips - 1)

    def partner(m):
        if chips & (chips - 1):
            return lax.rem(chip + m, chips)
        bits = [(1 << b, (m >> b) & 1) for b in range(chips.bit_length() - 1)]
        return sum(lax.rem(chip // size + bit, 2) * size for size, bit in bits)

    hops = range(chips - 1, 0, -1)

    def at_core():
        return (z, chip * 2 + 1 - core)

    def at_chip(other):
        return (z, other * 2 + core)

    def at_plane(other):
        return (other, me)

    def remote(src, dst, send, recv, to):
        return pltpu.make_async_remote_copy(
            src_ref=src, dst_ref=dst, send_sem=send, recv_sem=recv, device_id=to, device_id_type=MESH
        )

    def columns(head):
        return pl.ds(pl.multiple_of(head * SIZE, SIZE), SIZE)

    def round_columns(i):
        return pl.ds(pl.multiple_of(i * (chips * SIZE), SIZE), chips * SIZE)

    decay_load = pltpu.make_async_copy(d_any, d_ref, decay_s)
    decay_load.start()

    @pl.loop(0, own)
    def _(i):
        taken = round_columns(i)
        for j, src in enumerate((q_any, k_any, g_any, v_any)):
            pltpu.make_async_copy(src.at[:, taken], held.at[j, :, taken], load_s.at[i]).start()

    barrier = pltpu.get_barrier_semaphore()

    def greet(to):
        pl.semaphore_signal(barrier, inc=1, device_id=to, device_id_type=MESH)

    for step in range(1, planes):
        plane = lax.rem(z + step, planes)
        greet((plane, chip * 2 + lead_core(plane)))
    for m in hops:
        greet((z, partner(m) * 2 + lead_core(z)))
    greet(at_core())

    lower = lower_triangle(rows)
    row = lax.broadcasted_iota(jnp.int32, (rows, rows), 0)
    column = lax.broadcasted_iota(jnp.int32, (rows, rows), 1)
    upto = (row <= column).astype(F32).astype(BF16)
    after = (row > column).astype(F32).astype(BF16)
    ones = jnp.ones((rows, SIZE), BF16)
    row = lax.broadcasted_iota(jnp.int32, (heads, heads), 0)
    column = lax.broadcasted_iota(jnp.int32, (heads, heads), 1)
    owners = (column == (row % own) * chips + row // own).astype(F32).astype(BF16)

    decay_load.wait()
    decay = d_ref[...]
    decay_rows[...] = decay.astype(F32)
    by_owner = dot(dot(owners, decay).astype(BF16), ones)
    for o in range(chips):
        own_fin[o] = by_owner[o * own : (o + 1) * own]
    fin = dot(decay, ones)
    cumul = dot(decay, upto)
    forward_rows[...] = jnp.exp(cumul)
    backward_rows[...] = jnp.exp(fin - cumul)

    fin_copy = remote(own_fin, core_fin, fin_s, fin_r, at_core())

    def core_copies(begin, count, recv):
        taken = pl.ds(begin, count)
        return remote(terms.at[core, taken], from_core.at[taken], core_s, recv, at_core())

    def core_copy(i):
        return core_copies(i * chips, chips, core_r.at[i])

    def make_terms(head):
        taken = columns(head)
        keys = held[1, :, taken].T.astype(F32) * backward_rows[pl.ds(head, 1), :]
        terms[0, head] = dot(keys.astype(BF16), held[3, :, taken])
        queries = held[0, :, taken].T.astype(F32) * forward_rows[pl.ds(head, 1), :]
        terms[1, head] = dot(queries.astype(BF16), held[2, :, taken])

    def terms_step(i):
        part = held.at[:, :, round_columns(i)]
        pltpu.make_async_copy(part, part, load_s.at[i]).wait()
        for o in range(chips):
            make_terms(i * chips + o)

    def inside(head):
        taken = columns(head)
        query, key, grad, value = (held[j, :, taken] for j in range(4))
        picked = jnp.where(lower, decay_rows[pl.ds(head, 1), :], 0.0).astype(BF16)
        spans = dot(picked, jnp.concatenate([after, ones], axis=1))
        weights = jnp.where(lower, jnp.exp(spans[:, :rows]), 0.0)
        sums = spans[:, rows:]
        scales[0, head] = jnp.exp(sums)
        scales[1, head] = jnp.exp(own_fin[lax.rem(head, chips), pl.ds(head // chips, 1), :] - sums)
        probs = (over_columns(query, key) * weights).astype(BF16)
        grows = (over_columns(grad, value) * weights).astype(BF16)
        local[0, head] = dot(probs, value)
        local[1, head] = over_rows(probs, grad)
        local[2, head] = dot(grows, key)
        local[3, head] = over_rows(grows, query)

    def chip_fin_copy(other):
        return remote(
            chip_total.at[other], chip_fin.at[chip], chip_fs, chip_fr, at_chip(other)
        )

    def out_copy(i, other):
        to, slot = i * chips + other, i * chips + chip
        return remote(to_chips.at[to], from_chips.at[slot], out_s, out_r.at[i], at_chip(other))

    def out_copies(count, recv):
        taken = pl.ds(0, count)
        return remote(to_chips.at[taken], from_chips.at[taken], out_s, recv, at_core())

    def send_out(i, other):
        @pl.when(jnp.logical_not(last))
        def _():
            out_copy(i, other).start()

    def combine(i, send):
        core_copy(i).wait_recv()
        waiting = None
        for m in [*hops, 0]:
            other = partner(m) if m else chip
            head = i * chips + other
            factor = jnp.exp(own_fin[other, pl.ds(i, 1), :])
            total = (terms[kind, head] + factor * from_core[head]).astype(BF16)
            if m:
                to_chips[head] = total
            else:
                from_chips[head] = total
            if send and waiting is not None:
                send_out(i, waiting)
            waiting = other

    def plane_fin_copy(plane, side):
        to = (plane, chip * 2 + side)
        return remote(plane_fin.at[z], plane_fin.at[z], plane_fs, plane_fr, to)

    share_copy = remote(chip_fin, chip_fin, share_s, share_r, at_core())

    def planes_step(_):
        taken = chip_fin.at[pl.ds(0, chips - 1)]
        remote(taken, taken, chip_fs, chip_fr, at_core()).wait_recv()
        total = chip_fin[0]
        for other in range(1, chips):
            total = total + chip_fin[other]
        plane_fin[z] = total
        share_copy.start()
        for step in range(1, planes):
            for side in range(2):
                plane_fin_copy(lax.rem(z + step, planes), side).start()

    def plane_copy(i, other):
        return remote(
            plane_sum.at[i], from_planes.at[z, i], plane_s, plane_r.at[i], at_plane(other)
        )

    def factor_of(fins, at, i):
        return jnp.exp(fins[at, pl.ds(i, 1), :])

    def sum_step(i):
        fewer = (depth == planes - 1) & (spot < chips - 1)
        for few, count in ((fewer, chips - 2), (jnp.logical_not(fewer), chips - 1)):
            @pl.when(few)
            def _():
                out_copies(count, out_r.at[i]).wait_recv()

        @pl.when(depth < planes - 1)
        def _():
            total = from_chips[i * chips + place(0)].astype(F32)
            for j in range(1, chips):
                at = place(j)
                total = total * factor_of(chip_fin, at, i) + from_chips[i * chips + at].astype(F32)
            plane_sum[i] = total.astype(BF16)

            @pl.loop(0, planes - 1 - depth)
            def _(j):
                plane_copy(i, level(planes - 1 - j)).start()

    def back_copy(i, other):
        to, slot = i * chips + other, i * chips + chip
        recv = back_r.at[i] if i < own - 1 else late_r.at[chip]
        return remote(to_back.at[to], raw.at[slot], back_s, recv, at_chip(other))

    def back_copies(count, recv):
        taken = pl.ds(0, count)
        return remote(to_back.at[taken], raw.at[taken], back_s, recv, at_core())

    def send_back(i, to_first):
        for m in hops:
            other = partner(m)
            wanted = (depth > 0) | (other != place(0))
            if to_first is not None:
                wanted = wanted & ((other == 0) if to_first else (other != 0))

            @pl.when(wanted)
            def _():
                back_copy(i, other).start()

    def carry_step(i, lag=0):
        head = i * chips + chip
        if i == 0:
            taken = plane_fin.at[pl.ds(0, planes - 1)]
            remote(taken, taken, plane_fs, plane_fr, at_core()).wait_recv()
        for count in range(1, planes):
            @pl.when(depth == count)
            def _():
                taken = from_planes.at[pl.ds(0, count), i]
                remote(taken, taken, plane_s, plane_r.at[i], at_core()).wait_recv()

        def add_plane(j, state):
            at = level(j)
            return state * factor_of(plane_fin, at, i) + from_planes[at, i].astype(F32)

        state = lax.fori_loop(0, depth, add_plane, jnp.zeros((SIZE, SIZE), F32))
        for j in range(chips):
            at = place(j)
            to_back[i * chips + at] = state.astype(BF16)
            if j < chips - 1:
                state = state * factor_of(chip_fin, at, i) + from_chips[i * chips + at].astype(F32)
        if lag == 0:
            send_back(i, None)
        else:
            send_back(i, True)
            if i >= lag:
                send_back(i - lag, False)
            if i == own - 1:
                for late in range(max(own - lag, 0), own):
                    send_back(late, False)
        raw[head] = to_back[head]

    def last_part(i, other):
        head = i * chips + other
        return remote(raw.at[head], states.at[head], last_s, load_s.at[i], at_core())

    def last_copy(i):
        taken = pl.ds(i * chips, chips)
        return remote(raw.at[taken], states.at[taken], last_s, load_s.at[i], at_core())

    def apply(which, head, state):
        def put(j, taken, value):
            out_ref[j + which, :, taken] = value

        apply_state(which, head, columns(head), state, held, scales, local, put)

    def pass_step(i, late):
        if i < own - 1:
            @pl.when(jnp.logical_not(first))
            def _():
                back_copies(chips - 1, back_r.at[i]).wait_recv()
            last_copy(i).start()
        else:
            last_part(i, chip).start()
            for m in hops:
                other = partner(m)

                @pl.when(jnp.logical_not(first))
                def _():
                    back_copies(1, late_r.at[other]).wait_recv()
                last_part(i, other).start()
        for o in range(chips):
            head = i * chips + o
            factor = jnp.exp(core_fin[o, pl.ds(i, 1), :])
            state = (factor * raw[head].astype(F32) + from_core[head]).astype(BF16)
            if late and i == own - 1:
                states[head] = state
            else:
                apply(kind, head, state)

    def other_step(i, late):
        last_copy(i).wait_recv()
        if late and i == own - 1:
            return
        for o in range(chips):
            head = i * chips + o
            apply(core, head, states[head])

    @pl.when(first)
    def _():
        @pl.loop(0, heads)
        def _(head):
            raw[head] = jnp.zeros((SIZE, SIZE), BF16)

    parts = heads // 2

    def inside_step(part):
        for j in range(2):
            inside(part * 2 + j)

    def lead_turn(_):
        pl.semaphore_signal(go_s, inc=1, device_id=at_core(), device_id_type=MESH)

    def tail_turn(_):
        pl.semaphore_wait(go_s, 1)
        for i in range(own):
            for m in hops:
                send_out(i, partner(m))

    steps = {
        "planes": planes_step, "sum": sum_step, "carry": carry_step, "inside": inside_step,
    }

    @pl.when(lead)
    def _():
        half = own // 2
        pl.loop(0, half)(terms_step)
        pl.semaphore_wait(barrier, 2 * (chips + planes) - 3)
        fin_copy.start()
        for i in range(half):
            core_copy(i).start()
        fin_copy.wait_recv()
        chip_total[...] = own_fin[...] + core_fin[...]
        chip_fin[chip] = chip_total[chip]
        terms_step(half)
        core_copy(half).start()
        for m in hops:
            chip_fin_copy(partner(m)).start()
        combine(0, True)
        for i in range(half + 1, own):
            terms_step(i)
            core_copy(i).start()
            combine(i - half, True)
        for i in range(own - half, own):
            combine(i, True)
        front = {
            "turn": lead_turn, "pass": lambda i: pass_step(i, False),
            "other": lambda i: other_step(i, True),
        }
        for step, i in lead_plan(own, parts):
            {**steps, **front}[step](i)
        taken = chip_fin.at[pl.ds(0, chips - 1)]
        remote(taken, taken, chip_fs, chip_fr, at_core()).wait_send()
        share_copy.wait_send()
        for _ in range(2):
            taken = plane_fin.at[pl.ds(0, planes - 1)]
            remote(taken, taken, plane_fs, plane_fr, at_core()).wait_send()

    @pl.when(jnp.logical_not(lead))
    def _():
        pl.semaphore_wait(barrier, 1)
        fin_copy.start()

        @pl.loop(0, own)
        def _(i):
            terms_step(i)
            core_copy(i).start()

        fin_copy.wait_recv()
        tail = {
            "turn": tail_turn, "combine": lambda i: combine(i, False),
            "share": lambda _: share_copy.wait_recv(), "carry": lambda i: carry_step(i, LAG),
            "pass": lambda i: pass_step(i, True), "other": lambda i: other_step(i, False),
        }
        for step, i in tail_plan(own, parts):
            {**steps, **tail}[step](i)

    fin_copy.wait_send()
    core_copies(0, heads, core_r.at[0]).wait_send()

    @pl.when(jnp.logical_not(last))
    def _():
        out_copies(own * (chips - 1), out_r.at[0]).wait_send()
    fewer = (depth == 0) & (spot > 0)
    for few, count in ((fewer, chips - 2), (jnp.logical_not(fewer), chips - 1)):
        @pl.when(few)
        def _():
            back_copies(own * count, back_r.at[0]).wait_send()
    remote(raw, states, last_s, load_s.at[0], at_core()).wait_send()
    for count in range(1, planes):
        @pl.when(planes - 1 - depth == count)
        def _():
            taken = from_planes.at[pl.ds(0, count)]
            remote(taken, taken, plane_s, plane_r.at[0], at_core()).wait_send()


def computed(planes, devices, arrays):
    decay = pltpu.with_memory_space_constraint(arrays[-1].T, pltpu.HBM)
    arrays = [pltpu.with_memory_space_constraint(item, pltpu.HBM) for item in arrays[:-1]] + [decay]
    heads, rows = decay.shape
    chips = devices // 2
    own = heads // chips
    square = (SIZE, SIZE)
    wide = arrays[0].shape
    dma = pltpu.SemaphoreType.DMA
    return pl.pallas_call(
        functools.partial(main_kernel, planes, devices),
        out_shape=[
            jax.ShapeDtypeStruct((4,) + wide, BF16),
            jax.ShapeDtypeStruct((4,) + wide, BF16),
            jax.ShapeDtypeStruct((2, heads, rows, SIZE), F32),
            jax.ShapeDtypeStruct((4, heads) + square, F32),
            jax.ShapeDtypeStruct((heads,) + square, BF16),
        ],
        in_specs=[pl.BlockSpec(memory_space=pltpu.HBM)] * 5,
        out_specs=[pl.BlockSpec(memory_space=pltpu.VMEM)] * 5,
        scratch_shapes=[
            pltpu.VMEM((heads, rows), BF16),
            pltpu.VMEM((heads, rows), F32),
            pltpu.VMEM((heads, rows), F32),
            pltpu.VMEM((heads, rows), F32),
            pltpu.VMEM((2, heads) + square, F32),
            pltpu.VMEM((heads,) + square, F32),
            pltpu.VMEM((heads,) + square, BF16),
            pltpu.VMEM((heads,) + square, BF16),
            pltpu.VMEM((own,) + square, BF16),
            pltpu.VMEM((planes, own) + square, BF16),
            pltpu.VMEM((heads,) + square, BF16),
            pltpu.VMEM((heads,) + square, BF16),
            pltpu.VMEM((chips, own, SIZE), F32),
            pltpu.VMEM((chips, own, SIZE), F32),
            pltpu.VMEM((chips, own, SIZE), F32),
            pltpu.VMEM((chips, own, SIZE), F32),
            pltpu.VMEM((planes, own, SIZE), F32),
            dma((own,)), dma, pltpu.SemaphoreType.REGULAR, dma, dma, dma, dma, dma, dma, dma, dma,
            dma, dma((own,)), dma, dma((own,)), dma, dma((own,)),
            dma, dma((own,)), dma((chips,)), dma,
        ],
        compiler_params=pltpu.CompilerParams(
            collective_id=0, has_side_effects=True, vmem_limit_bytes=20 * 2**20
        ),
    )(*arrays)


def store_kernel(
    planes, chips, done, held, scales, local, states, o_out, dq_out, dk_out, dv_out, fresh, store_s
):
    heads = states.shape[0]
    width = chips * SIZE
    split = heads * SIZE - width
    which = late_kind(lax.axis_index("chain"), planes)
    outs = (o_out, dv_out, dq_out, dk_out)
    early, late = pl.ds(0, split), pl.ds(split, width)
    copies = [
        pltpu.make_async_copy(done.at[j, :, early], dst.at[:, early], store_s)
        for j, dst in enumerate(outs)
    ]
    for copy in copies:
        copy.start()

    def late_copies(kind):
        pairs = []
        for j in range(2):
            pairs.append((fresh.at[j], outs[2 * j + kind]))
            pairs.append((done.at[2 * j + 1 - kind, :, late], outs[2 * j + 1 - kind]))
        return [
            pltpu.make_async_copy(src, dst.at[:, late], store_s)
            for src, dst in pairs
        ]

    def put(j, taken, value):
        fresh[j // 2, :, taken] = value

    for o in range(chips):
        head = heads - chips + o
        apply_state(which, head, pl.ds(o * SIZE, SIZE), states[head], held, scales, local, put)
    for kind in range(2):
        @pl.when(which == kind)
        def _():
            for copy in late_copies(kind):
                copy.start()
    pltpu.make_async_copy(done, done, store_s).wait()


def stored(planes, chips, results):
    rows, features = results[0].shape[1:]
    return pl.pallas_call(
        functools.partial(store_kernel, planes, chips),
        out_shape=[jax.ShapeDtypeStruct((rows, features), BF16)] * 4,
        in_specs=[pl.BlockSpec(memory_space=pltpu.VMEM)] * 5,
        out_specs=[pl.BlockSpec(memory_space=pltpu.HBM)] * 4,
        scratch_shapes=[
            pltpu.VMEM((2, rows, chips * SIZE), BF16),
            pltpu.SemaphoreType.DMA,
        ],
        compiler_params=pltpu.CompilerParams(vmem_limit_bytes=4 * 2**20),
    )(*results)


def solution(mesh):
    planes, devices = mesh.shape["chain"], mesh.shape["inner"]

    def shards(*arrays):
        return tuple(stored(planes, devices // 2, computed(planes, devices, arrays)))

    spec = P(("chain", "inner"), None)
    return jax.shard_map(
        shards, mesh=mesh, in_specs=(spec,) * 5, out_specs=(spec,) * 4, check_vma=False
    )
```

```python
import functools

import jax
import jax.numpy as jnp
from jax import lax
from jax.experimental import pallas as pl
from jax.experimental.pallas import tpu as pltpu
from jax.sharding import PartitionSpec as P

SIZE = 128
F32 = jnp.float32
BF16 = jnp.bfloat16
MESH = pl.DeviceIdType.MESH
LAG = 1


def lower_triangle(rows):
    row = lax.broadcasted_iota(jnp.int32, (rows, rows), 0)
    column = lax.broadcasted_iota(jnp.int32, (rows, rows), 1)
    return row >= column


def over_rows(left, right):
    return lax.dot_general(left, right, (((0,), (0,)), ((), ())), preferred_element_type=F32)


def over_columns(left, right):
    return lax.dot_general(left, right, (((1,), (1,)), ((), ())), preferred_element_type=F32)


def dot(left, right):
    return jnp.dot(left, right, preferred_element_type=F32)


def plan(ready, rounds, parts, now):
    ready = sorted(ready)
    order, part = [], 0
    while ready:
        if ready[0][0] > now + 0.1 and part < parts:
            order.append(("inside", part))
            now += 10.0 / parts
            part += 1
            continue
        at, length, step, i = ready.pop(0)
        if step in ("pass", "other"):
            while part < min(parts, -(-parts * (i + 1) // rounds)):
                order.append(("inside", part))
                now += 10.0 / parts
                part += 1
        order.append((step, i))
        now = max(now, at) + length
    return order


def lead_plan(rounds, parts):
    ready = [(7.5, 0.1, "planes", 0)]
    for i in range(rounds):
        ready.append((7.8 + 0.7 * i, 0.15, "sum", i))
        ready.append((13.2 + 0.7 * i, 0.35, "carry", i))
        ready.append((19.0 + 0.7 * i, 0.55, "pass", i))
        ready.append((25.7 + 0.7 * i, 0.35, "other", i))
    turn = min(2, rounds - 1)
    ready.append((7.81 + 0.7 * turn, 0.01, "turn", 0))
    return plan(ready, rounds, parts, 6.7)


def tail_plan(rounds, parts):
    ready = [(7.9, 0.1, "turn", 0), (13.3, 0.05, "share", 0)]
    for i in range(rounds):
        ready.append((5.1 + 0.3 * i, 0.3, "combine", i))
        ready.append((13.4 + 0.7 * i, 0.15, "sum", i))
        ready.append((17.5 + 0.7 * i, 0.35, "carry", i))
        ready.append((24.6 + 0.7 * i, 0.55, "pass", i))
        ready.append((21.4 + 0.7 * i, 0.35, "other", i))
    return plan(ready, rounds, parts, 4.5)


def late_kind(plane, planes):
    return jnp.where(plane * 2 < planes, 1, 0)


def apply_state(which, head, place, state, held, scales, local, out_ref):
    taken = pl.ds(pl.multiple_of(head * SIZE, SIZE), SIZE)
    scale = scales[which, head]
    straight = dot(held[which, :, taken], state)
    out_ref(0, place, (local[which, head] + scale * straight).astype(BF16))
    turned = over_columns(held[2 + which, :, taken], state)
    out_ref(2, place, (local[2 + which, head] + scale * turned).astype(BF16))


def main_kernel(
    planes, devices, q_any, k_any, v_any, g_any, d_any, out_ref, held, scales, local, states,
    d_ref, decay_rows, forward_rows, backward_rows, terms, from_core,
    to_chips, from_chips, plane_sum, from_planes, to_back, raw,
    own_fin, core_fin, chip_total, chip_fin, plane_fin,
    load_s, decay_s, go_s, fin_s, fin_r, chip_fs, chip_fr, plane_fs, plane_fr, share_s, share_r,
    core_s, core_r, out_s, out_r, plane_s, plane_r, back_s, back_r, late_r, last_s,
):
    heads, rows = d_any.shape
    chips = devices // 2
    own = heads // chips
    z = lax.axis_index("chain")
    me = lax.axis_index("inner")
    chip, core = me // 2, lax.rem(me, 2)
    kind = 1 - core
    ahead = core == 1

    def place(j):
        return jnp.where(ahead, j, chips - 1 - j)

    def level(j):
        return jnp.where(ahead, j, planes - 1 - j)

    depth, spot = level(z), place(chip)

    def lead_core(plane):
        return late_kind(plane, planes)

    lead = core == lead_core(z)
    first = (depth == 0) & (spot == 0)
    last = (depth == planes - 1) & (spot == chips - 1)

    def partner(m):
        if chips & (chips - 1):
            return lax.rem(chip + m, chips)
        bits = [(1 << b, (m >> b) & 1) for b in range(chips.bit_length() - 1)]
        return sum(lax.rem(chip // size + bit, 2) * size for size, bit in bits)

    hops = range(chips - 1, 0, -1)

    def at_core():
        return (z, chip * 2 + 1 - core)

    def at_chip(other):
        return (z, other * 2 + core)

    def at_plane(other):
        return (other, me)

    def remote(src, dst, send, recv, to):
        return pltpu.make_async_remote_copy(
            src_ref=src, dst_ref=dst, send_sem=send, recv_sem=recv, device_id=to, device_id_type=MESH
        )

    def columns(head):
        return pl.ds(pl.multiple_of(head * SIZE, SIZE), SIZE)

    def round_columns(i):
        return pl.ds(pl.multiple_of(i * (chips * SIZE), SIZE), chips * SIZE)

    decay_load = pltpu.make_async_copy(d_any, d_ref, decay_s)
    decay_load.start()

    @pl.loop(0, own)
    def _(i):
        taken = round_columns(i)
        for j, src in enumerate((q_any, k_any, g_any, v_any)):
            pltpu.make_async_copy(src.at[:, taken], held.at[j, :, taken], load_s.at[i]).start()

    barrier = pltpu.get_barrier_semaphore()

    def greet(to):
        pl.semaphore_signal(barrier, inc=1, device_id=to, device_id_type=MESH)

    for step in range(1, planes):
        plane = lax.rem(z + step, planes)
        greet((plane, chip * 2 + lead_core(plane)))
    for m in hops:
        greet((z, partner(m) * 2 + lead_core(z)))
    greet(at_core())

    lower = lower_triangle(rows)
    row = lax.broadcasted_iota(jnp.int32, (rows, rows), 0)
    column = lax.broadcasted_iota(jnp.int32, (rows, rows), 1)
    upto = (row <= column).astype(F32).astype(BF16)
    after = (row > column).astype(F32).astype(BF16)
    ones = jnp.ones((rows, SIZE), BF16)
    row = lax.broadcasted_iota(jnp.int32, (heads, heads), 0)
    column = lax.broadcasted_iota(jnp.int32, (heads, heads), 1)
    owners = (column == (row % own) * chips + row // own).astype(F32).astype(BF16)

    decay_load.wait()
    decay = d_ref[...]
    decay_rows[...] = decay.astype(F32)
    by_owner = dot(dot(owners, decay).astype(BF16), ones)
    for o in range(chips):
        own_fin[o] = by_owner[o * own : (o + 1) * own]
    fin = dot(decay, ones)
    cumul = dot(decay, upto)
    forward_rows[...] = jnp.exp(cumul)
    backward_rows[...] = jnp.exp(fin - cumul)

    fin_copy = remote(own_fin, core_fin, fin_s, fin_r, at_core())

    def core_copies(begin, count, recv):
        taken = pl.ds(begin, count)
        return remote(terms.at[core, taken], from_core.at[taken], core_s, recv, at_core())

    def core_copy(i):
        return core_copies(i * chips, chips, core_r.at[i])

    def make_terms(head):
        taken = columns(head)
        keys = held[1, :, taken].T.astype(F32) * backward_rows[pl.ds(head, 1), :]
        terms[0, head] = dot(keys.astype(BF16), held[3, :, taken])
        queries = held[0, :, taken].T.astype(F32) * forward_rows[pl.ds(head, 1), :]
        terms[1, head] = dot(queries.astype(BF16), held[2, :, taken])

    def terms_step(i):
        part = held.at[:, :, round_columns(i)]
        pltpu.make_async_copy(part, part, load_s.at[i]).wait()
        for o in range(chips):
            make_terms(i * chips + o)

    def inside(head):
        taken = columns(head)
        query, key, grad, value = (held[j, :, taken] for j in range(4))
        picked = jnp.where(lower, decay_rows[pl.ds(head, 1), :], 0.0).astype(BF16)
        spans = dot(picked, jnp.concatenate([after, ones], axis=1))
        weights = jnp.where(lower, jnp.exp(spans[:, :rows]), 0.0)
        sums = spans[:, rows:]
        scales[0, head] = jnp.exp(sums)
        scales[1, head] = jnp.exp(own_fin[lax.rem(head, chips), pl.ds(head // chips, 1), :] - sums)
        probs = (over_columns(query, key) * weights).astype(BF16)
        grows = (over_columns(grad, value) * weights).astype(BF16)
        local[0, head] = dot(probs, value)
        local[1, head] = over_rows(probs, grad)
        local[2, head] = dot(grows, key)
        local[3, head] = over_rows(grows, query)

    def chip_fin_copy(other):
        return remote(
            chip_total.at[other], chip_fin.at[chip], chip_fs, chip_fr, at_chip(other)
        )

    def out_copy(i, other):
        to, slot = i * chips + other, i * chips + chip
        return remote(to_chips.at[to], from_chips.at[slot], out_s, out_r.at[i], at_chip(other))

    def out_copies(count, recv):
        taken = pl.ds(0, count)
        return remote(to_chips.at[taken], from_chips.at[taken], out_s, recv, at_core())

    def send_out(i, other):
        @pl.when(jnp.logical_not(last))
        def _():
            out_copy(i, other).start()

    def combine(i, send):
        core_copy(i).wait_recv()
        waiting = None
        for m in [*hops, 0]:
            other = partner(m) if m else chip
            head = i * chips + other
            factor = jnp.exp(own_fin[other, pl.ds(i, 1), :])
            total = (terms[kind, head] + factor * from_core[head]).astype(BF16)
            if m:
                to_chips[head] = total
            else:
                from_chips[head] = total
            if send and waiting is not None:
                send_out(i, waiting)
            waiting = other

    def plane_fin_copy(plane, side):
        to = (plane, chip * 2 + side)
        return remote(plane_fin.at[z], plane_fin.at[z], plane_fs, plane_fr, to)

    share_copy = remote(chip_fin, chip_fin, share_s, share_r, at_core())

    def planes_step(_):
        taken = chip_fin.at[pl.ds(0, chips - 1)]
        remote(taken, taken, chip_fs, chip_fr, at_core()).wait_recv()
        total = chip_fin[0]
        for other in range(1, chips):
            total = total + chip_fin[other]
        plane_fin[z] = total
        share_copy.start()
        for step in range(1, planes):
            for side in range(2):
                plane_fin_copy(lax.rem(z + step, planes), side).start()

    def plane_copy(i, other):
        return remote(
            plane_sum.at[i], from_planes.at[z, i], plane_s, plane_r.at[i], at_plane(other)
        )

    def factor_of(fins, at, i):
        return jnp.exp(fins[at, pl.ds(i, 1), :])

    def sum_step(i):
        fewer = (depth == planes - 1) & (spot < chips - 1)
        for few, count in ((fewer, chips - 2), (jnp.logical_not(fewer), chips - 1)):
            @pl.when(few)
            def _():
                out_copies(count, out_r.at[i]).wait_recv()

        @pl.when(depth < planes - 1)
        def _():
            total = from_chips[i * chips + place(0)].astype(F32)
            for j in range(1, chips):
                at = place(j)
                total = total * factor_of(chip_fin, at, i) + from_chips[i * chips + at].astype(F32)
            plane_sum[i] = total.astype(BF16)

            @pl.loop(0, planes - 1 - depth)
            def _(j):
                plane_copy(i, level(planes - 1 - j)).start()

    def back_copy(i, other):
        to, slot = i * chips + other, i * chips + chip
        recv = back_r.at[i] if i < own - 1 else late_r.at[chip]
        return remote(to_back.at[to], raw.at[slot], back_s, recv, at_chip(other))

    def back_copies(count, recv):
        taken = pl.ds(0, count)
        return remote(to_back.at[taken], raw.at[taken], back_s, recv, at_core())

    def send_back(i, to_first):
        for m in hops:
            other = partner(m)
            wanted = (depth > 0) | (other != place(0))
            if to_first is not None:
                wanted = wanted & ((other == 0) if to_first else (other != 0))

            @pl.when(wanted)
            def _():
                back_copy(i, other).start()

    def carry_step(i, lag=0):
        head = i * chips + chip
        if i == 0:
            taken = plane_fin.at[pl.ds(0, planes - 1)]
            remote(taken, taken, plane_fs, plane_fr, at_core()).wait_recv()
        for count in range(1, planes):
            @pl.when(depth == count)
            def _():
                taken = from_planes.at[pl.ds(0, count), i]
                remote(taken, taken, plane_s, plane_r.at[i], at_core()).wait_recv()

        def add_plane(j, state):
            at = level(j)
            return state * factor_of(plane_fin, at, i) + from_planes[at, i].astype(F32)

        state = lax.fori_loop(0, depth, add_plane, jnp.zeros((SIZE, SIZE), F32))
        for j in range(chips):
            at = place(j)
            to_back[i * chips + at] = state.astype(BF16)
            if j < chips - 1:
                state = state * factor_of(chip_fin, at, i) + from_chips[i * chips + at].astype(F32)
        if lag == 0:
            send_back(i, None)
        else:
            send_back(i, True)
            if i >= lag:
                send_back(i - lag, False)
            if i == own - 1:
                for late in range(max(own - lag, 0), own):
                    send_back(late, False)
        raw[head] = to_back[head]

    def last_part(i, other):
        head = i * chips + other
        return remote(raw.at[head], states.at[head], last_s, load_s.at[i], at_core())

    def last_copy(i):
        taken = pl.ds(i * chips, chips)
        return remote(raw.at[taken], states.at[taken], last_s, load_s.at[i], at_core())

    def apply(which, head, state):
        def put(j, taken, value):
            out_ref[j + which, :, taken] = value

        apply_state(which, head, columns(head), state, held, scales, local, put)

    def pass_step(i, late):
        if i < own - 1:
            @pl.when(jnp.logical_not(first))
            def _():
                back_copies(chips - 1, back_r.at[i]).wait_recv()
            last_copy(i).start()
        else:
            last_part(i, chip).start()
            for m in hops:
                other = partner(m)

                @pl.when(jnp.logical_not(first))
                def _():
                    back_copies(1, late_r.at[other]).wait_recv()
                last_part(i, other).start()
        for o in range(chips):
            head = i * chips + o
            factor = jnp.exp(core_fin[o, pl.ds(i, 1), :])
            state = (factor * raw[head].astype(F32) + from_core[head]).astype(BF16)
            if late and i == own - 1:
                states[head] = state
            else:
                apply(kind, head, state)

    def other_step(i, late):
        last_copy(i).wait_recv()
        if late and i == own - 1:
            return
        for o in range(chips):
            head = i * chips + o
            apply(core, head, states[head])

    @pl.when(first)
    def _():
        @pl.loop(0, heads)
        def _(head):
            raw[head] = jnp.zeros((SIZE, SIZE), BF16)

    parts = heads // 2

    def inside_step(part):
        for j in range(2):
            inside(part * 2 + j)

    def lead_turn(_):
        pl.semaphore_signal(go_s, inc=1, device_id=at_core(), device_id_type=MESH)

    def tail_turn(_):
        pl.semaphore_wait(go_s, 1)
        for i in range(own):
            for m in hops:
                send_out(i, partner(m))

    steps = {
        "planes": planes_step, "sum": sum_step, "carry": carry_step, "inside": inside_step,
    }

    @pl.when(lead)
    def _():
        half = own // 2
        pl.loop(0, half)(terms_step)
        pl.semaphore_wait(barrier, 2 * (chips + planes) - 3)
        fin_copy.start()
        for i in range(half):
            core_copy(i).start()
        fin_copy.wait_recv()
        chip_total[...] = own_fin[...] + core_fin[...]
        chip_fin[chip] = chip_total[chip]
        terms_step(half)
        core_copy(half).start()
        for m in hops:
            chip_fin_copy(partner(m)).start()
        combine(0, True)
        for i in range(half + 1, own):
            terms_step(i)
            core_copy(i).start()
            combine(i - half, True)
        for i in range(own - half, own):
            combine(i, True)
        front = {
            "turn": lead_turn, "pass": lambda i: pass_step(i, False),
            "other": lambda i: other_step(i, True),
        }
        for step, i in lead_plan(own, parts):
            {**steps, **front}[step](i)
        taken = chip_fin.at[pl.ds(0, chips - 1)]
        remote(taken, taken, chip_fs, chip_fr, at_core()).wait_send()
        share_copy.wait_send()
        for _ in range(2):
            taken = plane_fin.at[pl.ds(0, planes - 1)]
            remote(taken, taken, plane_fs, plane_fr, at_core()).wait_send()

    @pl.when(jnp.logical_not(lead))
    def _():
        pl.semaphore_wait(barrier, 1)
        fin_copy.start()

        @pl.loop(0, own)
        def _(i):
            terms_step(i)
            core_copy(i).start()

        fin_copy.wait_recv()
        tail = {
            "turn": tail_turn, "combine": lambda i: combine(i, False),
            "share": lambda _: share_copy.wait_recv(), "carry": lambda i: carry_step(i, LAG),
            "pass": lambda i: pass_step(i, True), "other": lambda i: other_step(i, False),
        }
        for step, i in tail_plan(own, parts):
            {**steps, **tail}[step](i)

    fin_copy.wait_send()
    core_copies(0, heads, core_r.at[0]).wait_send()

    @pl.when(jnp.logical_not(last))
    def _():
        out_copies(own * (chips - 1), out_r.at[0]).wait_send()
    fewer = (depth == 0) & (spot > 0)
    for few, count in ((fewer, chips - 2), (jnp.logical_not(fewer), chips - 1)):
        @pl.when(few)
        def _():
            back_copies(own * count, back_r.at[0]).wait_send()
    remote(raw, states, last_s, load_s.at[0], at_core()).wait_send()
    for count in range(1, planes):
        @pl.when(planes - 1 - depth == count)
        def _():
            taken = from_planes.at[pl.ds(0, count)]
            remote(taken, taken, plane_s, plane_r.at[0], at_core()).wait_send()


def computed(planes, devices, arrays):
    decay = pltpu.with_memory_space_constraint(arrays[-1].T, pltpu.HBM)
    arrays = [pltpu.with_memory_space_constraint(item, pltpu.HBM) for item in arrays[:-1]] + [decay]
    heads, rows = decay.shape
    chips = devices // 2
    own = heads // chips
    square = (SIZE, SIZE)
    wide = arrays[0].shape
    dma = pltpu.SemaphoreType.DMA
    return pl.pallas_call(
        functools.partial(main_kernel, planes, devices),
        out_shape=[
            jax.ShapeDtypeStruct((4,) + wide, BF16),
            jax.ShapeDtypeStruct((4,) + wide, BF16),
            jax.ShapeDtypeStruct((2, heads, rows, SIZE), F32),
            jax.ShapeDtypeStruct((4, heads) + square, F32),
            jax.ShapeDtypeStruct((heads,) + square, BF16),
        ],
        in_specs=[pl.BlockSpec(memory_space=pltpu.HBM)] * 5,
        out_specs=[pl.BlockSpec(memory_space=pltpu.VMEM)] * 5,
        scratch_shapes=[
            pltpu.VMEM((heads, rows), BF16),
            pltpu.VMEM((heads, rows), F32),
            pltpu.VMEM((heads, rows), F32),
            pltpu.VMEM((heads, rows), F32),
            pltpu.VMEM((2, heads) + square, F32),
            pltpu.VMEM((heads,) + square, F32),
            pltpu.VMEM((heads,) + square, BF16),
            pltpu.VMEM((heads,) + square, BF16),
            pltpu.VMEM((own,) + square, BF16),
            pltpu.VMEM((planes, own) + square, BF16),
            pltpu.VMEM((heads,) + square, BF16),
            pltpu.VMEM((heads,) + square, BF16),
            pltpu.VMEM((chips, own, SIZE), F32),
            pltpu.VMEM((chips, own, SIZE), F32),
            pltpu.VMEM((chips, own, SIZE), F32),
            pltpu.VMEM((chips, own, SIZE), F32),
            pltpu.VMEM((planes, own, SIZE), F32),
            dma((own,)), dma, pltpu.SemaphoreType.REGULAR, dma, dma, dma, dma, dma, dma, dma, dma,
            dma, dma((own,)), dma, dma((own,)), dma, dma((own,)),
            dma, dma((own,)), dma((chips,)), dma,
        ],
        compiler_params=pltpu.CompilerParams(
            collective_id=0, has_side_effects=True, vmem_limit_bytes=20 * 2**20
        ),
    )(*arrays)


def store_kernel(
    planes, chips, done, held, scales, local, states, o_out, dq_out, dk_out, dv_out, fresh, store_s
):
    heads = states.shape[0]
    width = chips * SIZE
    split = heads * SIZE - width
    which = late_kind(lax.axis_index("chain"), planes)
    outs = (o_out, dv_out, dq_out, dk_out)
    early, late = pl.ds(0, split), pl.ds(split, width)
    copies = [
        pltpu.make_async_copy(done.at[j, :, early], dst.at[:, early], store_s)
        for j, dst in enumerate(outs)
    ]
    for copy in copies:
        copy.start()

    def late_copies(kind):
        pairs = []
        for j in range(2):
            pairs.append((fresh.at[j], outs[2 * j + kind]))
            pairs.append((done.at[2 * j + 1 - kind, :, late], outs[2 * j + 1 - kind]))
        return [
            pltpu.make_async_copy(src, dst.at[:, late], store_s)
            for src, dst in pairs
        ]

    def put(j, taken, value):
        fresh[j // 2, :, taken] = value

    for o in range(chips):
        head = heads - chips + o
        apply_state(which, head, pl.ds(o * SIZE, SIZE), states[head], held, scales, local, put)
    for kind in range(2):
        @pl.when(which == kind)
        def _():
            for copy in late_copies(kind):
                copy.start()
    pltpu.make_async_copy(done, done, store_s).wait()


def stored(planes, chips, results):
    rows, features = results[0].shape[1:]
    return pl.pallas_call(
        functools.partial(store_kernel, planes, chips),
        out_shape=[jax.ShapeDtypeStruct((rows, features), BF16)] * 4,
        in_specs=[pl.BlockSpec(memory_space=pltpu.VMEM)] * 5,
        out_specs=[pl.BlockSpec(memory_space=pltpu.HBM)] * 4,
        scratch_shapes=[
            pltpu.VMEM((2, rows, chips * SIZE), BF16),
            pltpu.SemaphoreType.DMA,
        ],
        compiler_params=pltpu.CompilerParams(vmem_limit_bytes=4 * 2**20),
    )(*results)


def solution(mesh):
    planes, devices = mesh.shape["chain"], mesh.shape["inner"]

    def shards(*arrays):
        return tuple(stored(planes, devices // 2, computed(planes, devices, arrays)))

    spec = P(("chain", "inner"), None)
    return jax.shard_map(
        shards, mesh=mesh, in_specs=(spec,) * 5, out_specs=(spec,) * 4, check_vma=False
    )
```
